128 devices in a mesh: gx: 4 (over y), gy: 32 (over x, z, core).
Axes of the slice: x: 4, y: 4, z: 4, core: 2. Of those that a mesh axis runs over, the one named last changes fastest.
Arguments:
- element_fields: bfloat16 [65536, 5, 512], P(('gx', 'gy')), may hold values from -6 to 6
- ref_coords: float32 [3, 262144], P(None, ('gx', 'gy')), may hold values from -1 to 1
- local_element: int32 [262144], P(('gx', 'gy')), may hold values from 0 to 511
- owner: int32 [262144, 1], P(('gx', 'gy')), may hold values from 0 to 127; in each aligned block of 2048 rows (0 to 2047, 2048 to 4095, ...) at most 64 rows name the same one
- point_angle: float32 [262144], P(('gx', 'gy')), may hold values from -3.140625 to 3.140625
- point_axial: float32 [262144], P(('gx', 'gy')), may hold values from 0 to 8
- panel_weight: float32 [262144], P(('gx', 'gy')), may hold values from 0.5 to 2
- obs_radius: float32 [256], replicated, may hold values from 3 to 30
- obs_angle: float32 [256], replicated, may hold values from -3.140625 to 3.140625
- obs_axial: float32 [256], replicated, may hold values from -8 to 16
- step_phase: float32 [32], replicated, may hold values from -3.140625 to 3.140625
- observer_slot: int32 [256], replicated, may hold values from 0 to 255, each once
- prior_spectra: float32 [2, 32, 256], P(None, None, ('gx', 'gy')), may hold values from -6 to 6
Outputs:
- surface_values: float32 [5, 262144], P(None, ('gx', 'gy'))
- spectra: float32 [2, 32, 256], P(None, None, ('gx', 'gy'))
The draws below stay inside these ranges and needn't reach their ends.
Inputs may be any that keep to these rules, and one draw needn't show every extreme that they name: Among the points of one device at most 64 have the same owner, and in every draw some device has exactly 64 points owned by one device. `observer_slot`: each output column is named by exactly one observer.
All inputs are finite; a program needn't handle non-finite values.
Results may differ from the reference program's by a relative error of at most 0.0003.
Values sent between devices are 32-bit elements; how exact they have to be, the bound alone decides.
A program may use at most 64 MiB of HBM per device.

```python
import math
import jax
import jax.numpy as jnp
import numpy as np
from jax import lax

NODES = 512
FIELDS = 5
NOBS = 256
NFREQ = 32
ELEM_DEV = 512
PTS_DEV = 2048
ELEMENTS = 65536
POINTS = 262144
CAP = 64
DEVICES = 128


def plant(values, rng, low, high):
    extent = values.shape
    place = [jax.random.randint(jax.random.fold_in(rng, axis), (), 0, extent[axis]) for axis in range(len(extent))]
    values = values.at[tuple(place)].set(low)
    longest = extent.index(max(extent))
    place[longest] = (place[longest] + 1) % extent[longest]
    return values.at[tuple(place)].set(high)


def block_scale(key, shape, shards, low, top_value):
    factor_of, own = 1.0, jax.random.fold_in(key, 6)
    for axis_at, shards_of in shards:
        draws = jnp.exp(jax.random.uniform(jax.random.fold_in(own, axis_at), (shards_of,), jnp.float32, low / len(shards), top_value / len(shards)))
        factor_of = factor_of * jnp.repeat(draws, shape[axis_at] // shards_of).reshape([-1 if axis == axis_at else 1 for axis in range(len(shape))])
    return factor_of


def routed_block(key, own, number, rows, number_of, top, reach, slope):
    ranking = jax.random.permutation(key, number_of)
    heavy_load, usual = portions_of(number_of, rows * top, reach, slope, True), portions_of(number_of, rows * top, reach, slope, False)
    places = jnp.arange(number_of)

    def named(tallies, offset_by):
        used = int((tallies > 0).sum())
        fixed = max(1, used // 4)
        moved = fixed + (places - fixed + offset_by * (used - fixed)) % max(1, number_of - fixed)
        return jnp.zeros((number_of,), jnp.int32).at[ranking[jnp.where(places < fixed, places, moved)]].set(jnp.asarray(tallies, jnp.int32))

    tallies = jnp.where(number % 4 == 0, named(heavy_load, number // 4), named(usual, number - number // 4 - 1))
    mixed = jax.random.permutation(jax.random.fold_in(own, 3), number_of)
    giver, taker = mixed[0:number_of // 2 * 2:2], mixed[1:number_of // 2 * 2:2]
    margin = jnp.minimum(tallies[giver] - 1, reach - tallies[taker]) // 2
    margin = jnp.where((giver == ranking[0]) | (taker == ranking[0]) | (tallies[taker] == 0), 0, jnp.maximum(margin, 0))
    moved = jax.random.randint(jax.random.fold_in(own, 4), (number_of // 2,), 0, 1 << 20) % (margin + 1)
    tallies = tallies.at[giver].add(-moved).at[taker].add(moved)
    items = jnp.searchsorted(jnp.cumsum(tallies), jnp.arange(rows * top), side="right").astype(jnp.int32)
    listing = items.reshape(top, rows).T
    listing = listing[jax.random.permutation(jax.random.fold_in(own, 1), rows)]
    offset_by = jax.random.randint(jax.random.fold_in(own, 2), (rows, 1), 0, top)
    return jnp.take_along_axis(listing, (jnp.arange(top)[None, :] + offset_by) % top, axis=1)


def portions_of(amount, total, most, slope, full):
    loads = [(1 << 20) // math.isqrt(standing ** slope) + 1 for standing in range(1, amount + 1)]
    largest = most if full else min(most, max(-(-total // amount), total * loads[0] // sum(loads)))
    least = 1 if total - largest >= amount - 1 else 0
    holding, rest = [largest] + [least] * (amount - 1), total - largest - least * (amount - 1)
    while rest > 0:
        movable = [i for i in range(1, amount) if holding[i] < largest] or [i for i in range(1, amount) if holding[i] < most]
        mass, left = sum([loads[i] for i in movable]), rest
        for i in movable:
            extra = min(most - holding[i], max(1, left * loads[i] // mass), rest)
            holding[i] = holding[i] + extra
            rest = rest - extra
    return np.array(holding)


def normal_values(own_key, dims, width, bound, shards=(), kind=jnp.bfloat16):
    result = jax.random.normal(own_key, dims, jnp.float32) * width
    if len(shards) > 0:
        result = block_scale(own_key, dims, shards, -0.22, 0.18) * result
    return jnp.clip(result, min=-bound, max=bound).astype(kind)


def setup_inputs(seed: int = 0) -> dict:
    arg_keys = jax.random.split(jax.random.key(seed), 14)
    element_fields = normal_values(arg_keys[0], (ELEMENTS, FIELDS, NODES), 1.0, 6.0, ((0, 128),))
    ref_coords = jnp.clip(jax.random.uniform(arg_keys[1], (3, POINTS), jnp.float32, -1.0, 1.0) * block_scale(arg_keys[1], (3, POINTS), ((1, 128),), -0.4, 0.0), -1.0, 1.0)
    local_element = plant(jax.random.randint(arg_keys[2], (POINTS,), 0, ELEM_DEV), jax.random.fold_in(arg_keys[2], 1), 0, ELEM_DEV - 1).astype(jnp.int32)
    owner_keys = jax.random.split(jax.random.fold_in(arg_keys[3], 1), POINTS // PTS_DEV)
    owner_turns = jax.random.permutation(jax.random.fold_in(arg_keys[3], 3), POINTS // PTS_DEV)
    owner = jax.vmap(lambda own, number: routed_block(jax.random.fold_in(arg_keys[3], 2), own, number, PTS_DEV, DEVICES, 1, CAP, 2))(owner_keys, owner_turns).reshape((POINTS, 1))
    point_angle = jnp.clip(jax.random.uniform(arg_keys[4], (POINTS,), jnp.float32, -3.140625, 3.140625), -3.140625, 3.140625)
    point_axial = jnp.clip(8.0 * jax.random.uniform(arg_keys[5], (POINTS,), jnp.float32) ** block_scale(arg_keys[5], (POINTS,), ((0, 128),), -0.2, 0.2), 0.0, 8.0)
    panel_weight = jnp.clip(jnp.exp(math.log(2.0) - 1.3862944 * jax.random.uniform(arg_keys[6], (POINTS,), jnp.float32) ** block_scale(arg_keys[6], (POINTS,), ((0, 128),), -0.2, 0.2)), 0.5, 2.0)
    obs_radius = jnp.clip(jnp.exp(jax.random.uniform(arg_keys[7], (NOBS,), jnp.float32, math.log(3.0), math.log(30.0))), 3.0, 30.0)
    obs_angle = jnp.clip(jax.random.uniform(arg_keys[8], (NOBS,), jnp.float32, -3.140625, 3.140625), -3.140625, 3.140625)
    obs_axial = jnp.clip(jax.random.uniform(arg_keys[9], (NOBS,), jnp.float32, -8.0, 16.0), -8.0, 16.0)
    step_phase = jnp.clip(jax.random.uniform(arg_keys[10], (NFREQ,), jnp.float32, -3.140625, 3.140625), -3.140625, 3.140625)
    observer_slot = jax.random.permutation(arg_keys[11], NOBS).astype(jnp.int32)
    prior_spectra = normal_values(arg_keys[12], (2, NFREQ, NOBS), 1.0, 6.0, ((2, 128),), jnp.float32)
    return dict(element_fields=element_fields, ref_coords=ref_coords, local_element=local_element, owner=owner, point_angle=point_angle, point_axial=point_axial, panel_weight=panel_weight, obs_radius=obs_radius, obs_angle=obs_angle, obs_axial=obs_axial, step_phase=step_phase, observer_slot=observer_slot, prior_spectra=prior_spectra)


gll_nodes = np.array([-1.0, -0.8717401485096066, -0.5917001814331423, -0.2092992179024789, 0.2092992179024789, 0.5917001814331423, 0.8717401485096066, 1.0])
omega_base = 0.25

def lagrange(coord):
    columns = []
    for first in range(8):
        product = jnp.ones_like(coord)
        divisor = 1.0
        for second in range(8):
            if second != first:
                product = product * (coord - float(gll_nodes[second]))
                divisor = divisor * (gll_nodes[first] - gll_nodes[second])
        columns.append(product * float(1.0 / divisor))
    return jnp.stack(columns)

def node_weights(coords):
    along_r = lagrange(coords[0])
    along_s = lagrange(coords[1])
    along_t = lagrange(coords[2])
    pair_rs = along_r[:, None, :] * along_s[None, :, :]
    return (pair_rs[:, :, None, :] * along_t[None, None, :, :]).reshape(512, coords.shape[1])

def interpolate(fields, elem_ids, coords):
    weights = node_weights(coords)
    gathered = jnp.take(fields, elem_ids, axis=0).astype(jnp.float32)
    return jnp.einsum('nfq,qn->fn', gathered, weights)

def spectra_terms(values, angle, axial, weight, obs_radius, obs_angle, obs_axial, step_phase, norm_scale):
    cos_p = jnp.cos(angle)
    sin_p = jnp.sin(angle)
    step_x = (obs_radius * jnp.cos(obs_angle))[None, :] - cos_p[:, None]
    step_y = (obs_radius * jnp.sin(obs_angle))[None, :] - sin_p[:, None]
    step_z = obs_axial[None, :] - axial[:, None]
    distance = jnp.sqrt(step_x * step_x + step_y * step_y + step_z * step_z)
    density = values[0]
    vel_x = values[1]
    vel_y = values[2]
    vel_z = values[3]
    pressure = values[4]
    mass_flux = density * (vel_x * cos_p + vel_y * sin_p)
    radial = (step_x * cos_p[:, None] + step_y * sin_p[:, None]) / distance
    radial_vel = (vel_x[:, None] * step_x + vel_y[:, None] * step_y + vel_z[:, None] * step_z) / distance
    amplitude = weight[:, None] * (mass_flux[:, None] + pressure[:, None] * radial + mass_flux[:, None] * radial_vel) * obs_radius[None, :] / distance * norm_scale
    harmonic = omega_base * jnp.arange(1, step_phase.shape[0] + 1, dtype=jnp.float32)
    phases = distance[:, :, None] * harmonic[None, None, :] + step_phase[None, None, :]
    cos_sum = lax.optimization_barrier(jnp.sum(amplitude[:, :, None] * jnp.cos(phases), axis=0)).T
    sin_sum = -lax.optimization_barrier(jnp.sum(amplitude[:, :, None] * jnp.sin(phases), axis=0)).T
    return jnp.stack([cos_sum, sin_sum])

def reference(element_fields, ref_coords, local_element, owner, point_angle, point_axial, panel_weight, obs_radius, obs_angle, obs_axial, step_phase, observer_slot, prior_spectra):
    global_ids = (owner[:, 0] * ELEM_DEV + local_element).astype(jnp.int32)
    block_rows = math.gcd(POINTS, 2048)
    block_count = POINTS // block_rows

    def sample(pieces):
        return interpolate(element_fields, pieces[0], pieces[1])
    sampled = lax.map(sample, (global_ids.reshape(block_count, block_rows), ref_coords.reshape(3, block_count, block_rows).transpose(1, 0, 2)))
    surface_values = sampled.transpose(1, 0, 2).reshape(FIELDS, POINTS)
    norm_scale = 1.0 / math.sqrt(POINTS)

    def accumulate(running, pieces):
        return (running + spectra_terms(pieces[0], pieces[1], pieces[2], pieces[3], obs_radius, obs_angle, obs_axial, step_phase, norm_scale), None)
    starting = jnp.zeros((2, NFREQ, NOBS), jnp.float32)
    summed, unused = lax.scan(accumulate, starting, (surface_values.reshape(FIELDS, block_count, block_rows).transpose(1, 0, 2), point_angle.reshape(block_count, block_rows), point_axial.reshape(block_count, block_rows), panel_weight.reshape(block_count, block_rows)))
    placed = jnp.zeros_like(summed).at[:, :, observer_slot].set(summed)
    return (surface_values, prior_spectra + placed)
```

```python
import math

import jax
import jax.numpy as jnp
import numpy as np
from jax import lax
from jax.experimental import pallas as pl
from jax.experimental.pallas import tpu as pltpu
from jax.sharding import PartitionSpec as P

MESH = pl.DeviceIdType.MESH
F32 = jnp.float32
BF16 = jnp.bfloat16

DEV = 128
INNER = 32
CAP = 64
PTS = 2048
ELEM = 512
NODES = 512
FIELDS = 5
NOBS = 256
NFREQ = 32
BLK = 256

GLL = [
    -1.0,
    -0.8717401485096066,
    -0.5917001814331423,
    -0.2092992179024789,
    0.2092992179024789,
    0.5917001814331423,
    0.8717401485096066,
    1.0,
]
CENTRES = ((3, 2), (10, 4), (19, 4), (28, 4))


def fit_sincos():
    r = np.cos((np.arange(400) + 0.5) * np.pi / 400) * (np.pi / 2)
    x = r * r
    cheb = np.polynomial.chebyshev
    top = (np.pi / 2) ** 2

    def poly(y, degree):
        fitted = cheb.Chebyshev.fit(x, y, degree, domain=[0, top])
        return [float(v) for v in fitted.convert(kind=np.polynomial.Polynomial).coef]

    return poly(np.sin(r) / r, 5), poly(np.cos(r), 5)


SIN_C, COS_C = fit_sincos()
PI_HI = 3.140625
PI_LO = math.pi - 3.140625


def horner(coefs, x):
    total = coefs[-1] * x + coefs[-2]
    for value in coefs[-3::-1]:
        total = total * x + value
    return total


def sincos_twice(r):
    x = r * r
    s = horner(SIN_C, x) * r
    c = horner(COS_C, x)
    t = s + s
    return 1.0 - t * s, t * c


def lagrange(coord):
    gaps = [coord - node for node in GLL]
    left = [None, gaps[0]]
    for i in range(2, 8):
        left.append(left[-1] * gaps[i - 1])
    right = [None] * 8
    right[6] = gaps[7]
    for i in range(5, -1, -1):
        right[i] = right[i + 1] * gaps[i + 1]
    values = []
    for i in range(8):
        divisor = 1.0
        for m in range(8):
            if m != i:
                divisor *= GLL[i] - GLL[m]
        scale = float(1.0 / divisor)
        if i == 0:
            product = right[0]
        elif i == 7:
            product = left[7]
        else:
            product = left[i] * right[i]
        values.append(product * scale)
    return values


def split2(x):
    hi = x.astype(BF16)
    lo = (x - hi.astype(F32)).astype(BF16)
    return hi, lo


def split3(x):
    hi = x.astype(BF16)
    rest = x - hi.astype(F32)
    mid = rest.astype(BF16)
    lo = (rest - mid.astype(F32)).astype(BF16)
    return hi, mid, lo


def dot_nt(a, b):
    return lax.dot_general(a, b, (((1,), (1,)), ((), ())), preferred_element_type=F32)


def dot_nn(a, b):
    return lax.dot_general(a, b, (((1,), (0,)), ((), ())), preferred_element_type=F32)


def kernel(
    tab_hbm,
    coords_ref,
    local_ref,
    owner_ref,
    angle_ref,
    axial_ref,
    weight_ref,
    orad_ref,
    oang_ref,
    oax_ref,
    phase_ref,
    slot_ref,
    prior_ref,
    surf_ref,
    spec_ref,
    tab,
    tabt,
    hot,
    rankm,
    req_out,
    req_in,
    rid,
    lag,
    valt,
    rep_out,
    rep_in,
    cols,
    coefs,
    amp,
    inv_ref,
    ys,
    xs,
    sums,
    red_out,
    red_in,
    tab_sem,
    sems,
):
    me = lax.axis_index("gx") * INNER + lax.axis_index("gy")

    def target(d):
        flat = lax.rem(me + d, DEV)
        return flat, (flat // INNER, lax.rem(flat, INNER))

    tab_copy = pltpu.make_async_copy(tab_hbm, tab, tab_sem)
    tab_copy.start()
    barrier = pltpu.get_barrier_semaphore()

    @pl.loop(1, DEV)
    def _(d):
        flat, where = target(d)
        pl.semaphore_signal(barrier, inc=1, device_id=where, device_id_type=MESH)

    def exchange(source, landing, k, own, back=False):
        @pl.loop(1, DEV)
        def _(d):
            flat, where = target(DEV - d if back else d)
            pltpu.make_async_remote_copy(
                src_ref=source.at[flat if own else d],
                dst_ref=landing.at[d],
                send_sem=sems.at[2 * k],
                recv_sem=sems.at[2 * k + 1],
                device_id=where,
                device_id_type=MESH,
            ).start()

    def whole(landing, k):
        rest = landing.at[pl.ds(1, DEV - 1)]
        flat, where = target(1)
        return pltpu.make_async_remote_copy(
            src_ref=rest,
            dst_ref=rest,
            send_sem=sems.at[2 * k],
            recv_sem=sems.at[2 * k + 1],
            device_id=where,
            device_id_type=MESH,
        )

    rel = owner_ref[...] - me
    rel = jnp.where(rel < 0, rel + DEV, rel)
    dev_iota = lax.broadcasted_iota(jnp.int32, (DEV, BLK), 0)
    cap_iota = lax.broadcasted_iota(jnp.int32, (CAP, BLK), 0)
    before = jnp.where(
        lax.broadcasted_iota(jnp.int32, (BLK, BLK), 0) < lax.broadcasted_iota(jnp.int32, (BLK, BLK), 1),
        1.0,
        0.0,
    ).astype(BF16)
    offset = jnp.zeros((DEV, 1), F32)
    packed = jnp.zeros((DEV, 4 * CAP), F32)
    for blk in range(PTS // BLK):
        at = slice(blk * BLK, (blk + 1) * BLK)
        onehot = jnp.where(dev_iota == rel[:, at], 1.0, 0.0)
        onehot16 = onehot.astype(BF16)
        hot[0:DEV, at] = onehot16
        hot[DEV : 2 * DEV, at] = onehot16
        within = dot_nn(onehot16, before)
        rank = jnp.sum(onehot * (within + offset), axis=0, keepdims=True)
        offset = offset + jnp.sum(onehot, axis=1, keepdims=True)
        mask = cap_iota == rank.astype(jnp.int32)
        rankm[:, at] = jnp.where(mask, 1.0, 0.0)
        rows = [local_ref[:, at].astype(F32)] + [coords_ref[v : v + 1, at] for v in range(3)]
        pieces = [split3(row) for row in rows]
        for part in range(3):
            table = jnp.concatenate(
                [jnp.where(mask, pieces[v][part].astype(F32), 0.0) for v in range(4)], axis=0
            ).astype(BF16)
            packed = packed + dot_nt(onehot16, table)
    req_out[:, 0, :] = packed[:, 0:128]
    req_out[:, 1, :] = packed[:, 128:256]

    pl.semaphore_wait(barrier, DEV - 1)
    exchange(req_out, req_in, 0, False)
    req_in[0] = req_out[0]

    tab_copy.wait()
    for f in range(FIELDS):
        tabt[f * NODES : (f + 1) * NODES, :] = tab[f].T

    cos_p, sin_p = sincos_twice(angle_ref[...] * 0.5)
    axial = axial_ref[...]
    zero = jnp.zeros((5, PTS), F32)
    cols[...] = jnp.concatenate([cos_p, sin_p, axial, zero], axis=0).T
    cos_o, sin_o = sincos_twice(oang_ref[...] * 0.5)
    orad = orad_ref[...]
    obs_x = orad * cos_o
    obs_y = orad * sin_o
    obs_z = oax_ref[...]

    @pl.loop(0, PTS // 16)
    def _(step):
        rows = pl.ds(pl.multiple_of(step * 16, 16), 16)
        own = cols[rows, :]
        px = own[:, 0:1]
        py = own[:, 1:2]
        pz = own[:, 2:3]
        for g in range(2):
            lanes = slice(g * 128, (g + 1) * 128)
            dx = obs_x[:, lanes] - px
            dy = obs_y[:, lanes] - py
            dz = obs_z[:, lanes] - pz
            square = dx * dx + dy * dy + dz * dz
            inv = lax.rsqrt(square)
            dist = square * inv
            turns = jnp.round(dist * (0.125 / math.pi))
            r = dist * 0.125 - turns * PI_HI - turns * PI_LO
            c1, s1 = sincos_twice(r)
            t = c1 + c1
            c2 = t * c1 - 1.0
            s2 = t * s1
            c3 = t * c2 - c1
            s3 = t * s2 - s1
            c4 = t * c3 - c2
            s4 = t * s3 - s2
            c5 = t * c4 - c3
            s5 = t * s4 - s3
            t5 = c5 + c5
            c10 = t5 * c5 - 1.0
            s10 = t5 * s5
            c9 = t5 * c4 - c1
            t9 = c9 + c9
            c19 = t9 * c10 - c1
            s19 = t9 * s10 - s1
            c28 = t9 * c19 - c10
            s28 = t9 * s19 - s10
            inv_ref[rows, lanes] = inv
            for n, value in enumerate((c1, s1, c2, s2, c3, s3, c4, s4)):
                ys[n, rows, lanes] = value
            for n, value in enumerate((c10, s10, c19, s19, c28, s28)):
                xs[n, rows, lanes] = value

    whole(req_in, 0).wait_recv()

    first = req_in[:, 0, :].T
    second = req_in[:, 1, :].T
    rid[...] = first[0:CAP]
    for n, value in enumerate((first[CAP : 2 * CAP], second[0:CAP], second[CAP : 2 * CAP])):
        for i, weight in enumerate(lagrange(value)):
            lag[:, n * 8 + i, :] = weight

    elem_iota = lax.broadcasted_iota(jnp.int32, (ELEM, 128), 0).astype(F32)

    @pl.loop(0, CAP // 2)
    def _(pair):
        picks = []
        weights = []
        for half in range(2):
            c = pair * 2 + half
            picks.append(jnp.where(elem_iota == rid[pl.ds(c, 1), :], 1.0, 0.0).astype(BF16))
            weights.append(lag[c])
        pick = jnp.concatenate(picks, axis=1)
        weight = jnp.concatenate(weights, axis=1)
        for f in range(FIELDS):
            nodal = dot_nn(tabt[f * NODES : (f + 1) * NODES, :], pick)
            total = None
            for i in range(8):
                inner = None
                for j in range(8):
                    at = (i * 8 + j) * 8
                    term = nodal[at : at + 8, :] * weight[8 + j : 9 + j, :]
                    inner = term if inner is None else inner + term
                inner = inner * weight[i : i + 1, :]
                total = inner if total is None else total + inner
            value = jnp.sum(total * weight[16:24, :], axis=0, keepdims=True)
            valt[pl.ds(f * CAP + pair * 2, 1), :] = value[:, 0:128]
            valt[pl.ds(f * CAP + pair * 2 + 1, 1), :] = value[:, 128:256]

    valt[FIELDS * CAP : 384, :] = jnp.zeros((384 - FIELDS * CAP, 128), F32)
    for n in range(3):
        rep_out[:, n, :] = valt[n * 128 : (n + 1) * 128, :].T
    exchange(rep_out, rep_in, 1, False, back=True)
    rep_in[0] = rep_out[0]
    whole(rep_in, 1).wait_recv()

    parts = [split2(rep_in[:, n, :].T) for n in range(3)]
    table = jnp.concatenate(
        [
            jnp.concatenate([hi for hi, lo in parts], axis=0),
            jnp.concatenate([lo for hi, lo in parts], axis=0),
        ],
        axis=1,
    )
    for blk in range(PTS // BLK):
        at = slice(blk * BLK, (blk + 1) * BLK)
        candidates = dot_nn(table, hot[:, at])
        mask = rankm[:, at]
        for f in range(FIELDS):
            surf_ref[f : f + 1, at] = jnp.sum(
                candidates[f * CAP : (f + 1) * CAP, :] * mask, axis=0, keepdims=True
            )

    density = surf_ref[0:1, :]
    vel_x = surf_ref[1:2, :]
    vel_y = surf_ref[2:3, :]
    vel_z = surf_ref[3:4, :]
    pressure = surf_ref[4:5, :]
    normal = vel_x * cos_p + vel_y * sin_p
    scaled = weight_ref[...] * (1.0 / math.sqrt(PTS * DEV))
    flux = density * normal * scaled
    pressure = pressure * scaled
    coefs[...] = jnp.concatenate(
        [
            flux,
            pressure * cos_p + flux * vel_x,
            pressure * sin_p + flux * vel_y,
            flux * vel_z,
            -(pressure + flux * (normal + vel_z * axial)),
            jnp.zeros((3, PTS), F32),
        ],
        axis=0,
    ).T

    @pl.loop(0, PTS // 32)
    def _(step):
        rows = pl.ds(pl.multiple_of(step * 32, 32), 32)
        own = coefs[rows, :]
        for g in range(2):
            lanes = slice(g * 128, (g + 1) * 128)
            inv = inv_ref[rows, lanes]
            linear = (
                own[:, 1:2] * obs_x[:, lanes]
                + own[:, 2:3] * obs_y[:, lanes]
                + own[:, 3:4] * obs_z[:, lanes]
                + own[:, 4:5]
            )
            amp[rows, lanes] = (own[:, 0:1] + linear * inv) * (inv * orad[:, lanes])

    UNROLL = 8
    for g in range(2):
        lanes = slice(g * 128, (g + 1) * 128)
        for number, (centre, reach) in enumerate(CENTRES):

            def body(step, acc, number=number, reach=reach, lanes=lanes):
                acc = list(acc)
                for u in range(UNROLL):
                    rows = pl.ds(pl.multiple_of(step * (8 * UNROLL) + u * 8, 8), 8)
                    a = amp[rows, lanes]
                    if number == 0:
                        ac = a * ys[4, rows, lanes]
                        as_ = a * ys[5, rows, lanes]
                    else:
                        ac = a * xs[2 * number - 2, rows, lanes]
                        as_ = a * xs[2 * number - 1, rows, lanes]
                    acc[0] = acc[0] + ac
                    acc[1] = acc[1] + as_
                    for b in range(reach):
                        yc = ys[2 * b, rows, lanes]
                        ysn = ys[2 * b + 1, rows, lanes]
                        acc[2 + 4 * b] = acc[2 + 4 * b] + ac * yc
                        acc[3 + 4 * b] = acc[3 + 4 * b] + as_ * ysn
                        acc[4 + 4 * b] = acc[4 + 4 * b] + as_ * yc
                        acc[5 + 4 * b] = acc[5 + 4 * b] + ac * ysn
                return tuple(acc)

            start = tuple(jnp.zeros((8, 128), F32) for _ in range(2 + 4 * reach))
            acc = lax.fori_loop(0, PTS // (8 * UNROLL), body, start)

            def put(k, cosine, sine, lanes=lanes):
                sums[k - 1 : k, lanes] = jnp.sum(cosine, axis=0, keepdims=True)
                sums[NFREQ + k - 1 : NFREQ + k, lanes] = jnp.sum(sine, axis=0, keepdims=True)

            put(centre, acc[0], acc[1])
            for b in range(reach):
                p1, p2, p3, p4 = acc[2 + 4 * b : 6 + 4 * b]
                put(centre + b + 1, p1 - p2, p3 + p4)
                put(centre - b - 1, p1 + p2, p3 - p4)

    slot = slot_ref[...]
    col_iota = lax.broadcasted_iota(jnp.int32, (DEV, NOBS), 0) * 2
    pieces = split3(sums[...])
    placed = []
    for parity in range(2):
        choose = jnp.where(col_iota + parity == slot, 1.0, 0.0).astype(BF16)
        placed.append(dot_nt(choose, pieces[0]) + dot_nt(choose, pieces[1]) + dot_nt(choose, pieces[2]))
    red_out[:, 0, :] = jnp.concatenate(placed, axis=1)
    exchange(red_out, red_in, 2, True)
    red_in[0] = red_out[me]
    cos_f, sin_f = sincos_twice(phase_ref[...] * 0.5)
    whole(red_in, 2).wait_recv()
    total = jnp.sum(red_in[:, 0, :], axis=0, keepdims=True)
    for parity in range(2):
        cosine = total[:, parity * 64 : parity * 64 + 32]
        sine = total[:, parity * 64 + 32 : parity * 64 + 64]
        spec_ref[0, parity : parity + 1, :] = prior_ref[0, parity : parity + 1, :] + (
            cos_f * cosine - sin_f * sine
        )
        spec_ref[1, parity : parity + 1, :] = prior_ref[1, parity : parity + 1, :] - (
            sin_f * cosine + cos_f * sine
        )
    whole(req_in, 0).wait_send()
    whole(rep_in, 1).wait_send()
    whole(red_in, 2).wait_send()


def on_device(
    element_fields,
    ref_coords,
    local_element,
    owner,
    point_angle,
    point_axial,
    panel_weight,
    obs_radius,
    obs_angle,
    obs_axial,
    step_phase,
    observer_slot,
    prior_spectra,
):
    vmem = pl.BlockSpec(memory_space=pltpu.VMEM)
    surface, spectra = pl.pallas_call(
        kernel,
        out_shape=(
            jax.ShapeDtypeStruct((FIELDS, PTS), F32),
            jax.ShapeDtypeStruct((2, 2, NFREQ), F32),
        ),
        in_specs=[pl.BlockSpec(memory_space=pl.ANY)] + [vmem] * 12,
        out_specs=(vmem, vmem),
        scratch_shapes=[
            pltpu.VMEM((FIELDS, ELEM, NODES), BF16),
            pltpu.VMEM((FIELDS * NODES, ELEM), BF16),
            pltpu.VMEM((2 * DEV, PTS), BF16),
            pltpu.VMEM((CAP, PTS), F32),
            pltpu.VMEM((DEV, 2, 128), F32),
            pltpu.VMEM((DEV, 2, 128), F32),
            pltpu.VMEM((CAP, 128), F32),
            pltpu.VMEM((CAP, 24, 128), F32),
            pltpu.VMEM((384, 128), F32),
            pltpu.VMEM((DEV, 3, 128), F32),
            pltpu.VMEM((DEV, 3, 128), F32),
            pltpu.VMEM((PTS, 8), F32),
            pltpu.VMEM((PTS, 8), F32),
            pltpu.VMEM((PTS, NOBS), F32),
            pltpu.VMEM((PTS, NOBS), F32),
            pltpu.VMEM((8, PTS, NOBS), F32),
            pltpu.VMEM((6, PTS, NOBS), F32),
            pltpu.VMEM((2 * NFREQ, NOBS), F32),
            pltpu.VMEM((DEV, 1, 128), F32),
            pltpu.VMEM((DEV, 1, 128), F32),
            pltpu.SemaphoreType.DMA,
            pltpu.SemaphoreType.DMA((6,)),
        ],
        compiler_params=pltpu.CompilerParams(
            collective_id=0, has_side_effects=True, vmem_limit_bytes=63 * 1024 * 1024
        ),
        name="flow",
    )(
        element_fields.transpose(1, 0, 2),
        ref_coords,
        local_element.reshape(1, PTS),
        owner.reshape(1, PTS),
        point_angle.reshape(1, PTS),
        point_axial.reshape(1, PTS),
        panel_weight.reshape(1, PTS),
        obs_radius.reshape(1, NOBS),
        obs_angle.reshape(1, NOBS),
        obs_axial.reshape(1, NOBS),
        step_phase.reshape(1, NFREQ),
        observer_slot.reshape(1, NOBS),
        prior_spectra.transpose(0, 2, 1),
    )
    return surface, spectra.transpose(0, 2, 1)


def solution(mesh):
    return jax.shard_map(
        on_device,
        mesh=mesh,
        in_specs=(
            P(("gx", "gy"), None, None),
            P(None, ("gx", "gy")),
            P(("gx", "gy")),
            P(("gx", "gy"), None),
            P(("gx", "gy")),
            P(("gx", "gy")),
            P(("gx", "gy")),
            P(),
            P(),
            P(),
            P(),
            P(),
            P(None, None, ("gx", "gy")),
        ),
        out_specs=(P(None, ("gx", "gy")), P(None, None, ("gx", "gy"))),
        check_vma=False,
    )
```

```python
import math

import jax
import jax.numpy as jnp
import numpy as np
from jax import lax
from jax.experimental import pallas as pl
from jax.experimental.pallas import tpu as pltpu
from jax.sharding import PartitionSpec as P

LOGICAL = pl.DeviceIdType.LOGICAL
F32 = jnp.float32
BF16 = jnp.bfloat16

DEV = 128
INNER = 32
CAP = 64
PTS = 2048
ELEM = 512
NODES = 512
FIELDS = 5
NOBS = 256
NFREQ = 32
BLK = 256
WIDE = 4

GLL = [
    -1.0,
    -0.8717401485096066,
    -0.5917001814331423,
    -0.2092992179024789,
    0.2092992179024789,
    0.5917001814331423,
    0.8717401485096066,
    1.0,
]
CENTRES = ((3, 2), (10, 4), (19, 4), (28, 4))


def fit_sincos():
    r = np.cos((np.arange(400) + 0.5) * np.pi / 400) * (np.pi / 2)
    x = r * r
    cheb = np.polynomial.chebyshev
    top = (np.pi / 2) ** 2

    def poly(y, degree):
        fitted = cheb.Chebyshev.fit(x, y, degree, domain=[0, top])
        return [float(v) for v in fitted.convert(kind=np.polynomial.Polynomial).coef]

    return poly(np.sin(r) / r, 5), poly(np.cos(r), 5)


SIN_C, COS_C = fit_sincos()
PI_HI = 3.140625
PI_LO = math.pi - 3.140625


def horner(coefs, x):
    total = coefs[-1] * x + coefs[-2]
    for value in coefs[-3::-1]:
        total = total * x + value
    return total


def sincos_twice(r):
    x = r * r
    s = horner(SIN_C, x) * r
    c = horner(COS_C, x)
    t = s + s
    return 1.0 - t * s, t * c


def lagrange(coord):
    gaps = [coord - node for node in GLL]
    left = [None, gaps[0]]
    for i in range(2, 8):
        left.append(left[-1] * gaps[i - 1])
    right = [None] * 8
    right[6] = gaps[7]
    for i in range(5, -1, -1):
        right[i] = right[i + 1] * gaps[i + 1]
    values = []
    for i in range(8):
        divisor = 1.0
        for m in range(8):
            if m != i:
                divisor *= GLL[i] - GLL[m]
        scale = float(1.0 / divisor)
        if i == 0:
            product = right[0]
        elif i == 7:
            product = left[7]
        else:
            product = left[i] * right[i]
        values.append(product * scale)
    return values


def split2(x):
    hi = x.astype(BF16)
    lo = (x - hi.astype(F32)).astype(BF16)
    return hi, lo


def split3(x):
    hi = x.astype(BF16)
    rest = x - hi.astype(F32)
    mid = rest.astype(BF16)
    lo = (rest - mid.astype(F32)).astype(BF16)
    return hi, mid, lo


def products(left, right, mine, theirs):
    a = [piece.astype(F32) for piece in split3(mine)]
    b = [piece.astype(F32) for piece in split3(theirs)]
    for i in range(3):
        for j in range(3 - i):
            left.append(a[i])
            right.append(b[j])


def dot_nt(a, b):
    return lax.dot_general(a, b, (((1,), (1,)), ((), ())), preferred_element_type=F32)


def dot_nn(a, b):
    return lax.dot_general(a, b, (((1,), (0,)), ((), ())), preferred_element_type=F32)


def kernel(
    tab_hbm,
    coords_ref,
    local_ref,
    owner_ref,
    angle_ref,
    axial_ref,
    weight_ref,
    orad_ref,
    oang_ref,
    oax_ref,
    phase_ref,
    slot_ref,
    prior_ref,
    surf_ref,
    spec_ref,
    tab,
    tabt,
    hot,
    rankm,
    req_out,
    req_in,
    rid,
    lag,
    valt,
    rep_out,
    rep_in,
    square_ref,
    amp,
    geo,
    sums,
    red_out,
    red_in,
    tab_sem,
    sems,
):
    me = lax.axis_index("gx") * INNER + lax.axis_index("gy")

    def target(d):
        return lax.rem(me + d, DEV)

    def others(body):
        @pl.loop(0, 18)
        def _(step):
            for u in range(7):
                body(step * 7 + (u + 1))

        body(DEV - 1)

    tab_copy = pltpu.make_async_copy(tab_hbm, tab, tab_sem)
    tab_copy.start()
    barrier = pltpu.get_barrier_semaphore()
    others(lambda d: pl.semaphore_signal(barrier, inc=1, device_id=target(d), device_id_type=LOGICAL))

    def exchange(source, landing, k, own, back=False):
        def send(d):
            flat = target(DEV - d if back else d)
            pltpu.make_async_remote_copy(
                src_ref=source.at[flat if own else d],
                dst_ref=landing.at[d],
                send_sem=sems.at[2 * k],
                recv_sem=sems.at[2 * k + 1],
                device_id=flat,
                device_id_type=LOGICAL,
            ).start()

        others(send)

    def whole(landing, k):
        rest = landing.at[pl.ds(1, DEV - 1)]
        return pltpu.make_async_remote_copy(
            src_ref=rest,
            dst_ref=rest,
            send_sem=sems.at[2 * k],
            recv_sem=sems.at[2 * k + 1],
            device_id=target(1),
            device_id_type=LOGICAL,
        )

    rel = owner_ref[...] - me
    rel = jnp.where(rel < 0, rel + DEV, rel)
    dev_iota = lax.broadcasted_iota(jnp.int32, (DEV, BLK), 0)
    cap_iota = lax.broadcasted_iota(jnp.int32, (CAP, BLK), 0)
    before = jnp.where(
        lax.broadcasted_iota(jnp.int32, (BLK, BLK), 0) < lax.broadcasted_iota(jnp.int32, (BLK, BLK), 1),
        1.0,
        0.0,
    ).astype(BF16)
    offset = jnp.zeros((DEV, 1), F32)
    packed = jnp.zeros((DEV, 4 * CAP), F32)
    for blk in range(PTS // BLK):
        at = slice(blk * BLK, (blk + 1) * BLK)
        onehot = jnp.where(dev_iota == rel[:, at], 1.0, 0.0)
        onehot16 = onehot.astype(BF16)
        hot[0:DEV, at] = onehot16
        hot[DEV : 2 * DEV, at] = onehot16
        within = dot_nn(onehot16, before)
        rank = jnp.sum(onehot * (within + offset), axis=0, keepdims=True)
        offset = offset + jnp.sum(onehot, axis=1, keepdims=True)
        mask = cap_iota == rank.astype(jnp.int32)
        rankm[:, at] = jnp.where(mask, 1.0, 0.0)
        rows = [local_ref[:, at].astype(F32)] + [coords_ref[v : v + 1, at] for v in range(3)]
        pieces = [split3(row) for row in rows]
        for part in range(3):
            table = jnp.concatenate(
                [jnp.where(mask, pieces[v][part].astype(F32), 0.0) for v in range(4)], axis=0
            ).astype(BF16)
            packed = packed + dot_nt(onehot16, table)
    req_out[:, 0, :] = packed[:, 0:128]
    req_out[:, 1, :] = packed[:, 128:256]

    cos_p, sin_p = sincos_twice(angle_ref[...] * 0.5)
    axial = axial_ref[...]
    cos_o, sin_o = sincos_twice(oang_ref[...] * 0.5)
    orad = orad_ref[...]
    obs_x = orad * cos_o
    obs_y = orad * sin_o
    obs_z = oax_ref[...]
    mid_p = axial - 4.0
    mid_o = obs_z - 4.0
    left, right = [], []
    for mine, theirs in ((cos_p * -2.0, obs_x), (sin_p * -2.0, obs_y), (mid_p * -2.0, mid_o)):
        products(left, right, mine, theirs)
    one_p = jnp.ones((1, PTS), F32)
    one_o = jnp.ones((1, NOBS), F32)
    for piece in split3(mid_p * mid_p + 1.0):
        left.append(piece.astype(F32))
        right.append(one_o)
    for piece in split3(orad * orad + mid_o * mid_o):
        left.append(one_p)
        right.append(piece.astype(F32))
    square_ref[...] = dot_nn(jnp.concatenate(left, axis=0).T.astype(BF16), jnp.concatenate(right, axis=0).astype(BF16))
    tab_copy.wait()
    for f in range(FIELDS):
        tabt[f * NODES : (f + 1) * NODES, :] = tab[f].T

    pl.semaphore_wait(barrier, DEV - 1)
    exchange(req_out, req_in, 0, False)
    req_in[0] = req_out[0]

    def geometry(first, last):
        @pl.loop(first, last)
        def _(step):
            for u in range(2):
                blk = step * 2 + u
                for g in range(2):
                    square = square_ref[pl.ds(pl.multiple_of(blk * 8, 8), 8), g * 128 : (g + 1) * 128]
                    inv = lax.rsqrt(square)
                    dist = square * inv
                    turns = jnp.round(dist * (0.125 / math.pi))
                    r = dist * 0.125 - turns * PI_HI - turns * PI_LO
                    c1, s1 = sincos_twice(r)
                    t = c1 + c1
                    c2 = t * c1 - 1.0
                    s2 = t * s1
                    c3 = t * c2 - c1
                    s3 = t * s2 - s1
                    c4 = t * c3 - c2
                    s4 = t * s3 - s2
                    c5 = t * c4 - c3
                    s5 = t * s4 - s3
                    t5 = c5 + c5
                    c10 = t5 * c5 - 1.0
                    s10 = t5 * s5
                    c9 = t5 * c4 - c1
                    t9 = c9 + c9
                    c19 = t9 * c10 - c1
                    s19 = t9 * s10 - s1
                    c28 = t9 * c19 - c10
                    s28 = t9 * s19 - s10
                    for n, value in enumerate(
                        (c1, s1, c2, s2, c3, s3, c4, s4, c10, s10, c19, s19, c28, s28, inv)
                    ):
                        geo[blk, g, n] = value

    geometry(0, 52)

    whole(req_in, 0).wait_recv()

    first = req_in[:, 0, :].T
    second = req_in[:, 1, :].T
    rid[...] = first[0:CAP]
    for n, value in enumerate((first[CAP : 2 * CAP], second[0:CAP], second[CAP : 2 * CAP])):
        for i, weight in enumerate(lagrange(value)):
            lag[:, n * 8 + i, :] = weight

    elem_iota = lax.broadcasted_iota(jnp.int32, (ELEM, 128), 0).astype(F32)

    @pl.loop(0, CAP // WIDE)
    def _(group):
        picks = []
        weights = []
        for part in range(WIDE):
            c = group * WIDE + part
            picks.append(jnp.where(elem_iota == rid[pl.ds(c, 1), :], 1.0, 0.0).astype(BF16))
            weights.append(lag[c])
        pick = jnp.concatenate(picks, axis=1)
        weight = jnp.concatenate(weights, axis=1)
        for f in range(FIELDS):
            nodal = dot_nn(tabt[f * NODES : (f + 1) * NODES, :], pick)
            total = None
            for i in range(8):
                inner = None
                for j in range(8):
                    at = (i * 8 + j) * 8
                    term = nodal[at : at + 8, :] * weight[8 + j : 9 + j, :]
                    inner = term if inner is None else inner + term
                inner = inner * weight[i : i + 1, :]
                total = inner if total is None else total + inner
            value = jnp.sum(total * weight[16:24, :], axis=0, keepdims=True)
            for part in range(WIDE):
                valt[pl.ds(f * CAP + group * WIDE + part, 1), :] = value[:, part * 128 : (part + 1) * 128]

    valt[FIELDS * CAP : 384, :] = jnp.zeros((384 - FIELDS * CAP, 128), F32)
    for n in range(3):
        rep_out[:, n, :] = valt[n * 128 : (n + 1) * 128, :].T
    exchange(rep_out, rep_in, 1, False, back=True)
    rep_in[0] = rep_out[0]
    geometry(52, PTS // 16)
    whole(rep_in, 1).wait_recv()

    parts = [split2(rep_in[:, n, :].T) for n in range(3)]
    table = jnp.concatenate(
        [
            jnp.concatenate([hi for hi, lo in parts], axis=0),
            jnp.concatenate([lo for hi, lo in parts], axis=0),
        ],
        axis=1,
    )
    for blk in range(PTS // BLK):
        at = slice(blk * BLK, (blk + 1) * BLK)
        candidates = dot_nn(table, hot[:, at])
        mask = rankm[:, at]
        for f in range(FIELDS):
            surf_ref[f : f + 1, at] = jnp.sum(
                candidates[f * CAP : (f + 1) * CAP, :] * mask, axis=0, keepdims=True
            )

    density = surf_ref[0:1, :]
    vel_x = surf_ref[1:2, :]
    vel_y = surf_ref[2:3, :]
    vel_z = surf_ref[3:4, :]
    pressure = surf_ref[4:5, :]
    normal = vel_x * cos_p + vel_y * sin_p
    scaled = weight_ref[...] * (1.0 / math.sqrt(PTS * DEV))
    flux = density * normal * scaled
    pressure = pressure * scaled
    left, right = [], []
    products(left, right, pressure * cos_p + flux * vel_x, obs_x)
    products(left, right, pressure * sin_p + flux * vel_y, obs_y)
    products(left, right, flux * vel_z, obs_z)
    for piece in split3(-(pressure + flux * (normal + vel_z * axial))):
        left.append(piece.astype(F32))
        right.append(one_o)
    zero_o = jnp.zeros((1, NOBS), F32)
    other = [zero_o] * len(left)
    for piece in split3(flux):
        left.append(piece.astype(F32))
        right.append(zero_o)
        other.append(one_o)
    left = jnp.concatenate(left, axis=0).T.astype(BF16)
    right = jnp.concatenate(
        [jnp.concatenate(right, axis=0), jnp.concatenate(other, axis=0)], axis=1
    ).astype(BF16)
    for blk in range(PTS // BLK):
        mixed = dot_nn(left[blk * BLK : (blk + 1) * BLK, :], right)
        for n in range(BLK // 8):
            at = blk * (BLK // 8) + n
            for g in range(2):
                lanes = slice(g * 128, (g + 1) * 128)
                inv = geo[at, g, 14]
                linear = mixed[n * 8 : n * 8 + 8, lanes]
                amp[at, g] = (mixed[n * 8 : n * 8 + 8, 256 + g * 128 : 384 + g * 128] + linear * inv) * (
                    inv * orad[:, lanes]
                )

    UNROLL = 8
    for g in range(2):
        lanes = slice(g * 128, (g + 1) * 128)
        for number, (centre, reach) in enumerate(CENTRES):

            def body(step, acc, number=number, reach=reach, g=g):
                acc = list(acc)
                for u in range(UNROLL):
                    blk = step * UNROLL + u
                    a = amp[blk, g]
                    at = 4 if number == 0 else 6 + 2 * number
                    ac = a * geo[blk, g, at]
                    as_ = a * geo[blk, g, at + 1]
                    acc[0] = acc[0] + ac
                    acc[1] = acc[1] + as_
                    for b in range(reach):
                        yc = geo[blk, g, 2 * b]
                        ysn = geo[blk, g, 2 * b + 1]
                        acc[2 + 4 * b] = acc[2 + 4 * b] + ac * yc
                        acc[3 + 4 * b] = acc[3 + 4 * b] + as_ * ysn
                        acc[4 + 4 * b] = acc[4 + 4 * b] + as_ * yc
                        acc[5 + 4 * b] = acc[5 + 4 * b] + ac * ysn
                return tuple(acc)

            start = tuple(jnp.zeros((8, 128), F32) for _ in range(2 + 4 * reach))
            acc = lax.fori_loop(0, PTS // (8 * UNROLL), body, start)

            def put(k, cosine, sine, lanes=lanes):
                sums[k - 1 : k, lanes] = jnp.sum(cosine, axis=0, keepdims=True)
                sums[NFREQ + k - 1 : NFREQ + k, lanes] = jnp.sum(sine, axis=0, keepdims=True)

            put(centre, acc[0], acc[1])
            for b in range(reach):
                p1, p2, p3, p4 = acc[2 + 4 * b : 6 + 4 * b]
                put(centre + b + 1, p1 - p2, p3 + p4)
                put(centre - b - 1, p1 + p2, p3 - p4)

    slot = slot_ref[...]
    col_iota = lax.broadcasted_iota(jnp.int32, (DEV, NOBS), 0) * 2
    pieces = split3(sums[...])
    placed = []
    for parity in range(2):
        choose = jnp.where(col_iota + parity == slot, 1.0, 0.0).astype(BF16)
        placed.append(dot_nt(choose, pieces[0]) + dot_nt(choose, pieces[1]) + dot_nt(choose, pieces[2]))
    red_out[:, 0, :] = jnp.concatenate(placed, axis=1)
    exchange(red_out, red_in, 2, True)
    red_in[0] = red_out[me]
    cos_f, sin_f = sincos_twice(phase_ref[...] * 0.5)
    whole(red_in, 2).wait_recv()
    total = jnp.sum(red_in[:, 0, :], axis=0, keepdims=True)
    for parity in range(2):
        cosine = total[:, parity * 64 : parity * 64 + 32]
        sine = total[:, parity * 64 + 32 : parity * 64 + 64]
        spec_ref[0, parity : parity + 1, :] = prior_ref[0, parity : parity + 1, :] + (
            cos_f * cosine - sin_f * sine
        )
        spec_ref[1, parity : parity + 1, :] = prior_ref[1, parity : parity + 1, :] - (
            sin_f * cosine + cos_f * sine
        )
    whole(req_in, 0).wait_send()
    whole(rep_in, 1).wait_send()
    whole(red_in, 2).wait_send()


def on_device(
    element_fields,
    ref_coords,
    local_element,
    owner,
    point_angle,
    point_axial,
    panel_weight,
    obs_radius,
    obs_angle,
    obs_axial,
    step_phase,
    observer_slot,
    prior_spectra,
):
    vmem = pl.BlockSpec(memory_space=pltpu.VMEM)
    surface, spectra = pl.pallas_call(
        kernel,
        out_shape=(
            jax.ShapeDtypeStruct((FIELDS, PTS), F32),
            jax.ShapeDtypeStruct((2, 2, NFREQ), F32),
        ),
        in_specs=[pl.BlockSpec(memory_space=pl.ANY)] + [vmem] * 12,
        out_specs=(vmem, vmem),
        scratch_shapes=[
            pltpu.VMEM((FIELDS, ELEM, NODES), BF16),
            pltpu.VMEM((FIELDS * NODES, ELEM), BF16),
            pltpu.VMEM((2 * DEV, PTS), BF16),
            pltpu.VMEM((CAP, PTS), F32),
            pltpu.VMEM((DEV, 2, 128), F32),
            pltpu.VMEM((DEV, 2, 128), F32),
            pltpu.VMEM((CAP, 128), F32),
            pltpu.VMEM((CAP, 24, 128), F32),
            pltpu.VMEM((384, 128), F32),
            pltpu.VMEM((DEV, 3, 128), F32),
            pltpu.VMEM((DEV, 3, 128), F32),
            pltpu.VMEM((PTS, NOBS), F32),
            pltpu.VMEM((PTS // 8, 2, 8, 128), F32),
            pltpu.VMEM((PTS // 8, 2, 15, 8, 128), F32),
            pltpu.VMEM((2 * NFREQ, NOBS), F32),
            pltpu.VMEM((DEV, 1, 128), F32),
            pltpu.VMEM((DEV, 1, 128), F32),
            pltpu.SemaphoreType.DMA,
            pltpu.SemaphoreType.DMA((6,)),
        ],
        compiler_params=pltpu.CompilerParams(
            collective_id=0, has_side_effects=True, vmem_limit_bytes=63 * 1024 * 1024
        ),
        name="flow",
    )(
        element_fields.transpose(1, 0, 2),
        ref_coords,
        local_element.reshape(1, PTS),
        owner.reshape(1, PTS),
        point_angle.reshape(1, PTS),
        point_axial.reshape(1, PTS),
        panel_weight.reshape(1, PTS),
        obs_radius.reshape(1, NOBS),
        obs_angle.reshape(1, NOBS),
        obs_axial.reshape(1, NOBS),
        step_phase.reshape(1, NFREQ),
        observer_slot.reshape(1, NOBS),
        prior_spectra.transpose(0, 2, 1),
    )
    return surface, spectra.transpose(0, 2, 1)


def solution(mesh):
    return jax.shard_map(
        on_device,
        mesh=mesh,
        in_specs=(
            P(("gx", "gy"), None, None),
            P(None, ("gx", "gy")),
            P(("gx", "gy")),
            P(("gx", "gy"), None),
            P(("gx", "gy")),
            P(("gx", "gy")),
            P(("gx", "gy")),
            P(),
            P(),
            P(),
            P(),
            P(),
            P(None, None, ("gx", "gy")),
        ),
        out_specs=(P(None, ("gx", "gy")), P(None, None, ("gx", "gy"))),
        check_vma=False,
    )
```

```python
import math

import jax
import jax.numpy as jnp
import numpy as np
from jax import lax
from jax.experimental import pallas as pl
from jax.experimental.pallas import tpu as pltpu
from jax.sharding import PartitionSpec as P

LOGICAL = pl.DeviceIdType.LOGICAL
F32 = jnp.float32
BF16 = jnp.bfloat16

DEV = 128
INNER = 32
CAP = 64
PTS = 2048
ELEM = 512
NODES = 512
FIELDS = 5
NOBS = 256
NFREQ = 32
BLK = 256
WIDE = 8
UNROLL = 16
SOON = 48
SOON_PTS = PTS * SOON // CAP
DELTAS = sorted(
    [(a, b, c, d) for a in range(4) for b in range(4) for c in range(4) for d in range(2)][1:],
    key=lambda t: -sum(min(v, 4 - v) for v in t[:3]) - 0.3 * t[3],
)

GLL = [
    -1.0,
    -0.8717401485096066,
    -0.5917001814331423,
    -0.2092992179024789,
    0.2092992179024789,
    0.5917001814331423,
    0.8717401485096066,
    1.0,
]
CENTRES = ((3, 2), (10, 4), (19, 4), (28, 4))


def fit_sincos():
    r = np.cos((np.arange(400) + 0.5) * np.pi / 400) * (np.pi / 2)
    x = r * r
    cheb = np.polynomial.chebyshev
    top = (np.pi / 2) ** 2

    def poly(y, degree):
        fitted = cheb.Chebyshev.fit(x, y, degree, domain=[0, top])
        return [float(v) for v in fitted.convert(kind=np.polynomial.Polynomial).coef]

    return poly(np.sin(r) / r, 5), poly(np.cos(r), 5)


SIN_C, COS_C = fit_sincos()
PI_HI = 3.140625
PI_LO = math.pi - 3.140625


def horner(coefs, x):
    total = coefs[-1] * x + coefs[-2]
    for value in coefs[-3::-1]:
        total = total * x + value
    return total


def sincos_twice(r):
    x = r * r
    s = horner(SIN_C, x) * r
    c = horner(COS_C, x)
    t = s + s
    return 1.0 - t * s, t * c


def lagrange(coord):
    gaps = [coord - node for node in GLL]
    left = [None, gaps[0]]
    for i in range(2, 8):
        left.append(left[-1] * gaps[i - 1])
    right = [None] * 8
    right[6] = gaps[7]
    for i in range(5, -1, -1):
        right[i] = right[i + 1] * gaps[i + 1]
    values = []
    for i in range(8):
        divisor = 1.0
        for m in range(8):
            if m != i:
                divisor *= GLL[i] - GLL[m]
        scale = float(1.0 / divisor)
        if i == 0:
            product = right[0]
        elif i == 7:
            product = left[7]
        else:
            product = left[i] * right[i]
        values.append(product * scale)
    return values


def split2(x):
    hi = x.astype(BF16)
    lo = (x - hi.astype(F32)).astype(BF16)
    return hi, lo


def split3(x):
    hi = x.astype(BF16)
    rest = x - hi.astype(F32)
    mid = rest.astype(BF16)
    lo = (rest - mid.astype(F32)).astype(BF16)
    return hi, mid, lo


def products(left, right, mine, theirs):
    a = [piece.astype(F32) for piece in split3(mine)]
    b = [piece.astype(F32) for piece in split3(theirs)]
    for i in range(3):
        for j in range(3 - i):
            left.append(a[i])
            right.append(b[j])


def dot_nt(a, b):
    return lax.dot_general(a, b, (((1,), (1,)), ((), ())), preferred_element_type=F32)


def dot_nn(a, b):
    return lax.dot_general(a, b, (((1,), (0,)), ((), ())), preferred_element_type=F32)


def kernel(
    tab_hbm,
    coords_ref,
    local_ref,
    owner_ref,
    angle_ref,
    axial_ref,
    weight_ref,
    orad_ref,
    oang_ref,
    oax_ref,
    phase_ref,
    slot_ref,
    prior_ref,
    surf_ref,
    spec_ref,
    tab,
    tabt,
    hot,
    rankm,
    req_out,
    req_in,
    rid,
    lag,
    valt,
    valt_b,
    rep_out,
    rep_in,
    rep_out_b,
    rep_in_b,
    swap,
    hot_p,
    rankm_p,
    partial,
    square_ref,
    amp,
    geo,
    sums,
    red_out,
    red_in,
    tab_sem,
    sems,
):
    me = lax.axis_index("gx") * INNER + lax.axis_index("gy")

    y, x, z, core = me // 32, lax.rem(me // 8, 4), lax.rem(me // 2, 4), lax.rem(me, 2)

    def target(delta):
        dy, dx, dz, dc = delta
        return (
            lax.rem(y + dy, 4) * 32 + lax.rem(x + dx, 4) * 8 + lax.rem(z + dz, 4) * 2 + lax.rem(core + dc, 2)
        )

    def others(body):
        for delta in DELTAS:
            code = delta[0] * 32 + delta[1] * 8 + delta[2] * 2 + delta[3]
            body(code, target(delta), target(((4 - delta[0]) % 4, (4 - delta[1]) % 4, (4 - delta[2]) % 4, delta[3])))

    tab_copy = pltpu.make_async_copy(tab_hbm, tab, tab_sem)
    tab_copy.start()
    barrier = pltpu.get_barrier_semaphore()
    others(
        lambda code, there, back: pl.semaphore_signal(
            barrier, inc=1, device_id=there, device_id_type=LOGICAL
        )
    )

    def exchange(source, landing, k, own=False, reply=False):
        def send(code, there, back):
            pltpu.make_async_remote_copy(
                src_ref=source.at[there if own else code],
                dst_ref=landing.at[code],
                send_sem=sems.at[2 * k],
                recv_sem=sems.at[2 * k + 1],
                device_id=back if reply else there,
                device_id_type=LOGICAL,
            ).start()

        others(send)

    def whole(landing, k):
        rest = landing.at[pl.ds(1, DEV - 1)]
        return pltpu.make_async_remote_copy(
            src_ref=rest,
            dst_ref=rest,
            send_sem=sems.at[2 * k],
            recv_sem=sems.at[2 * k + 1],
            device_id=lax.rem(me + 1, DEV),
            device_id_type=LOGICAL,
        )

    own = owner_ref[...]
    rel = (
        ((own // 32 - y + 4) & 3) * 32
        + (((own // 8) & 3) - x + 4 & 3) * 8
        + (((own // 2) & 3) - z + 4 & 3) * 2
        + ((own & 1) - core + 2 & 1)
    )
    dev_iota = lax.broadcasted_iota(jnp.int32, (DEV, BLK), 0)
    cap_iota = lax.broadcasted_iota(jnp.int32, (CAP, BLK), 0)
    before = jnp.where(
        lax.broadcasted_iota(jnp.int32, (BLK, BLK), 0) < lax.broadcasted_iota(jnp.int32, (BLK, BLK), 1),
        1.0,
        0.0,
    ).astype(BF16)
    offset = jnp.zeros((DEV, 1), F32)
    packed = jnp.zeros((DEV, 4 * CAP), F32)
    swap_iota = lax.broadcasted_iota(jnp.int32, (PTS - SOON_PTS, BLK), 0)
    count = jnp.zeros((1, 1), F32)
    wrong = None
    ranks, swaps = [], []
    for blk in range(PTS // BLK):
        at = slice(blk * BLK, (blk + 1) * BLK)
        onehot = jnp.where(dev_iota == rel[:, at], 1.0, 0.0)
        onehot16 = onehot.astype(BF16)
        hot[0:DEV, at] = onehot16
        hot[DEV : 2 * DEV, at] = onehot16
        within = dot_nn(onehot16, before)
        rank = jnp.sum(onehot * (within + offset), axis=0, keepdims=True)
        offset = offset + jnp.sum(onehot, axis=1, keepdims=True)
        if blk * BLK == SOON_PTS:
            wrong = count
            count = jnp.zeros((1, 1), F32)
        flag = jnp.where(rank >= SOON if blk * BLK < SOON_PTS else rank < SOON, 1.0, 0.0)
        number = dot_nn(jnp.broadcast_to(flag, (8, BLK)).astype(BF16), before)[0:1] + count
        count = count + jnp.sum(flag, axis=1, keepdims=True)
        if wrong is not None:
            flag = jnp.where(number < wrong, flag, 0.0)
        number = jnp.where(flag > 0.5, number, -1.0).astype(jnp.int32)
        swap[:, at] = jnp.where(swap_iota == number, 1.0, 0.0).astype(BF16)
        ranks.append(rank)
        swaps.append(flag)
        mask = cap_iota == rank.astype(jnp.int32)
        rankm[:, at] = jnp.where(mask, 1.0, 0.0)
        rows = [local_ref[:, at].astype(F32)] + [coords_ref[v : v + 1, at] for v in range(3)]
        pieces = [split3(row) for row in rows]
        for part in range(3):
            table = jnp.concatenate(
                [jnp.where(mask, pieces[v][part].astype(F32), 0.0) for v in range(4)], axis=0
            ).astype(BF16)
            packed = packed + dot_nt(onehot16, table)
    req_out[:, 0, :] = packed[:, 0:128]
    req_out[:, 1, :] = packed[:, 128:256]

    cos_p, sin_p = sincos_twice(angle_ref[...] * 0.5)
    attributes = [piece.astype(F32) for row in (cos_p, sin_p, axial_ref[...], weight_ref[...]) for piece in split3(row)]
    attributes.append(rel.astype(F32))
    attributes.append(jnp.concatenate(ranks, axis=1))
    attributes.append(jnp.zeros((2, PTS), F32))
    attributes = jnp.concatenate(attributes, axis=0).astype(BF16)
    to_first = dot_nt(attributes[:, SOON_PTS:], swap[:, SOON_PTS:]).astype(BF16)
    to_last = dot_nt(attributes[:, :SOON_PTS], swap[:, :SOON_PTS]).astype(BF16)
    moved = jnp.concatenate(
        [dot_nn(to_first, swap[:, :SOON_PTS]), dot_nn(to_last, swap[:, SOON_PTS:])], axis=1
    )
    ordered = jnp.where(jnp.concatenate(swaps, axis=1) > 0.5, moved, attributes.astype(F32))
    cos_p, sin_p, axial, panel = [
        ordered[n : n + 1] + ordered[n + 1 : n + 2] + ordered[n + 2 : n + 3] for n in (0, 3, 6, 9)
    ]
    rel_p = ordered[12:13].astype(jnp.int32)
    rank_p = ordered[13:14].astype(jnp.int32)
    for blk in range(PTS // BLK):
        at = slice(blk * BLK, (blk + 1) * BLK)
        onehot16 = jnp.where(dev_iota == rel_p[:, at], 1.0, 0.0).astype(BF16)
        hot_p[0:DEV, at] = onehot16
        hot_p[DEV : 2 * DEV, at] = onehot16
        rankm_p[:, at] = jnp.where(cap_iota == rank_p[:, at], 1.0, 0.0)

    pl.semaphore_wait(barrier, DEV - 1)
    exchange(req_out, req_in, 0)
    req_in[0] = req_out[0]

    cos_o, sin_o = sincos_twice(oang_ref[...] * 0.5)
    orad = orad_ref[...]
    obs_x = orad * cos_o
    obs_y = orad * sin_o
    obs_z = oax_ref[...]
    mid_p = axial - 4.0
    mid_o = obs_z - 4.0
    left, right = [], []
    for mine, theirs in ((cos_p * -2.0, obs_x), (sin_p * -2.0, obs_y), (mid_p * -2.0, mid_o)):
        products(left, right, mine, theirs)
    one_p = jnp.ones((1, PTS), F32)
    one_o = jnp.ones((1, NOBS), F32)
    for piece in split3(mid_p * mid_p + 1.0):
        left.append(piece.astype(F32))
        right.append(one_o)
    for piece in split3(orad * orad + mid_o * mid_o):
        left.append(one_p)
        right.append(piece.astype(F32))
    square_ref[...] = dot_nn(jnp.concatenate(left, axis=0).T.astype(BF16), jnp.concatenate(right, axis=0).astype(BF16))
    tab_copy.wait()
    for f in range(FIELDS):
        tabt[f * NODES : (f + 1) * NODES, :] = tab[f].T

    def geometry(first, last):
        @pl.loop(first, last)
        def _(step):
            for u in range(2):
                blk = step * 2 + u
                for g in range(2):
                    square = square_ref[pl.ds(pl.multiple_of(blk * 8, 8), 8), g * 128 : (g + 1) * 128]
                    inv = lax.rsqrt(square)
                    dist = square * inv
                    turns = jnp.round(dist * (0.125 / math.pi))
                    r = dist * 0.125 - turns * PI_HI - turns * PI_LO
                    c1, s1 = sincos_twice(r)
                    t = c1 + c1
                    c2 = t * c1 - 1.0
                    s2 = t * s1
                    c3 = t * c2 - c1
                    s3 = t * s2 - s1
                    c4 = t * c3 - c2
                    s4 = t * s3 - s2
                    c5 = t * c4 - c3
                    s5 = t * s4 - s3
                    t5 = c5 + c5
                    c10 = t5 * c5 - 1.0
                    s10 = t5 * s5
                    c9 = t5 * c4 - c1
                    t9 = c9 + c9
                    c19 = t9 * c10 - c1
                    s19 = t9 * s10 - s1
                    c28 = t9 * c19 - c10
                    s28 = t9 * s19 - s10
                    for n, value in enumerate(
                        (c1, s1, c2, s2, c3, s3, c4, s4, c10, s10, c19, s19, c28, s28, inv)
                    ):
                        geo[blk, g, n] = value

    geometry(0, PTS // 16)

    whole(req_in, 0).wait_recv()

    first = req_in[:, 0, :].T
    second = req_in[:, 1, :].T
    rid[...] = first[0:CAP]
    for n, value in enumerate((first[CAP : 2 * CAP], second[0:CAP], second[CAP : 2 * CAP])):
        for i, weight in enumerate(lagrange(value)):
            lag[:, n * 8 + i, :] = weight

    elem_iota = lax.broadcasted_iota(jnp.int32, (ELEM, 128), 0).astype(F32)

    def gather(group, land, first, span):
        picks = []
        weights = []
        for part in range(WIDE):
            c = group * WIDE + part
            picks.append(jnp.where(elem_iota == rid[pl.ds(c, 1), :], 1.0, 0.0).astype(BF16))
            weights.append(lag[c])
        pick = jnp.concatenate(picks, axis=1)
        weight = jnp.concatenate(weights, axis=1)
        for f in range(FIELDS):
            nodal = dot_nn(tabt[f * NODES : (f + 1) * NODES, :], pick)
            total = None
            for i in range(8):
                inner = None
                for j in range(8):
                    at = (i * 8 + j) * 8
                    term = nodal[at : at + 8, :] * weight[8 + j : 9 + j, :]
                    inner = term if inner is None else inner + term
                inner = inner * weight[i : i + 1, :]
                total = inner if total is None else total + inner
            value = jnp.sum(total * weight[16:24, :], axis=0, keepdims=True)
            for part in range(WIDE):
                land[pl.ds(f * span + (group * WIDE - first) + part, 1), :] = value[:, part * 128 : (part + 1) * 128]

    pl.loop(0, SOON // WIDE)(lambda group: gather(group, valt, 0, SOON))
    valt[FIELDS * SOON : 256, :] = jnp.zeros((256 - FIELDS * SOON, 128), F32)
    for n in range(2):
        rep_out[:, n, :] = valt[n * 128 : (n + 1) * 128, :].T
    exchange(rep_out, rep_in, 1, reply=True)
    rep_in[0] = rep_out[0]
    pl.loop(SOON // WIDE, CAP // WIDE)(lambda group: gather(group, valt_b, SOON, CAP - SOON))
    valt_b[FIELDS * (CAP - SOON) : 128, :] = jnp.zeros((128 - FIELDS * (CAP - SOON), 128), F32)
    rep_out_b[:, 0, :] = valt_b[...].T
    exchange(rep_out_b, rep_in_b, 3, reply=True)
    rep_in_b[0] = rep_out_b[0]

    def sources(landing, count):
        parts = [split2(landing[:, n, :].T) for n in range(count)]
        return jnp.concatenate(
            [
                jnp.concatenate([hi for hi, lo in parts], axis=0),
                jnp.concatenate([lo for hi, lo in parts], axis=0),
            ],
            axis=1,
        )

    def pick(table, choose, mask, span):
        found = dot_nn(table, choose)
        return [
            jnp.sum(found[f * span : (f + 1) * span, :] * mask, axis=0, keepdims=True) for f in range(FIELDS)
        ]

    def amplitudes(first, last, values):
        at_p = slice(first * BLK, last * BLK)
        density, vel_x, vel_y, vel_z, pressure = values
        cos_q, sin_q, axial_q = cos_p[:, at_p], sin_p[:, at_p], axial[:, at_p]
        normal = vel_x * cos_q + vel_y * sin_q
        scaled = panel[:, at_p] * (1.0 / math.sqrt(PTS * DEV))
        flux = density * normal * scaled
        pressure = pressure * scaled
        left, right = [], []
        products(left, right, pressure * cos_q + flux * vel_x, obs_x)
        products(left, right, pressure * sin_q + flux * vel_y, obs_y)
        products(left, right, flux * vel_z, obs_z)
        for piece in split3(-(pressure + flux * (normal + vel_z * axial_q))):
            left.append(piece.astype(F32))
            right.append(one_o)
        zero_o = jnp.zeros((1, NOBS), F32)
        other = [zero_o] * len(left)
        for piece in split3(flux):
            left.append(piece.astype(F32))
            right.append(zero_o)
            other.append(one_o)
        left = jnp.concatenate(left, axis=0).T.astype(BF16)
        right = jnp.concatenate(
            [jnp.concatenate(right, axis=0), jnp.concatenate(other, axis=0)], axis=1
        ).astype(BF16)
        for blk in range(last - first):
            mixed = dot_nn(left[blk * BLK : (blk + 1) * BLK, :], right)
            for n in range(BLK // 8):
                at = (first + blk) * (BLK // 8) + n
                for g in range(2):
                    lanes = slice(g * 128, (g + 1) * 128)
                    inv = geo[at, g, 14]
                    linear = mixed[n * 8 : n * 8 + 8, lanes]
                    amp[at, g] = (
                        mixed[n * 8 : n * 8 + 8, 256 + g * 128 : 384 + g * 128] + linear * inv
                    ) * (inv * orad[:, lanes])

    def put(k, lanes, cosine, sine):
        sums[k - 1 : k, lanes] = jnp.sum(cosine, axis=0, keepdims=True)
        sums[NFREQ + k - 1 : NFREQ + k, lanes] = jnp.sum(sine, axis=0, keepdims=True)

    def green(first, last, begin, end):
        for g in range(2):
            lanes = slice(g * 128, (g + 1) * 128)
            base = 0
            for number, (centre, reach) in enumerate(CENTRES):

                def body(step, acc, number=number, reach=reach, g=g):
                    acc = list(acc)
                    for u in range(UNROLL):
                        blk = step * UNROLL + u
                        a = amp[blk, g]
                        at = 4 if number == 0 else 6 + 2 * number
                        ac = a * geo[blk, g, at]
                        as_ = a * geo[blk, g, at + 1]
                        acc[0] = acc[0] + ac
                        acc[1] = acc[1] + as_
                        for b in range(reach):
                            yc = geo[blk, g, 2 * b]
                            ysn = geo[blk, g, 2 * b + 1]
                            acc[2 + 4 * b] = acc[2 + 4 * b] + ac * yc
                            acc[3 + 4 * b] = acc[3 + 4 * b] + as_ * ysn
                            acc[4 + 4 * b] = acc[4 + 4 * b] + as_ * yc
                            acc[5 + 4 * b] = acc[5 + 4 * b] + ac * ysn
                    return tuple(acc)

                count = 2 + 4 * reach
                if begin:
                    start = tuple(jnp.zeros((8, 128), F32) for _ in range(count))
                else:
                    start = tuple(partial[g, base + n] for n in range(count))
                acc = lax.fori_loop(first // (8 * UNROLL), last // (8 * UNROLL), body, start)
                if end:
                    put(centre, lanes, acc[0], acc[1])
                    for b in range(reach):
                        p1, p2, p3, p4 = acc[2 + 4 * b : 6 + 4 * b]
                        put(centre + b + 1, lanes, p1 - p2, p3 + p4)
                        put(centre - b - 1, lanes, p1 + p2, p3 - p4)
                else:
                    for n in range(count):
                        partial[g, base + n] = acc[n]
                base += count

    whole(rep_in, 1).wait_recv()
    table = sources(rep_in, 2)
    soon_blocks = SOON_PTS // BLK
    found = []
    for blk in range(soon_blocks):
        at = slice(blk * BLK, (blk + 1) * BLK)
        found.append(pick(table, hot_p[:, at], rankm_p[0:SOON, at], SOON))
    amplitudes(0, soon_blocks, [jnp.concatenate([row[f] for row in found], axis=1) for f in range(FIELDS)])
    green(0, SOON_PTS, True, False)
    whole(rep_in_b, 3).wait_recv()
    table_b = sources(rep_in_b, 1)
    found = []
    for blk in range(soon_blocks, PTS // BLK):
        at = slice(blk * BLK, (blk + 1) * BLK)
        found.append(
            [
                one + two
                for one, two in zip(
                    pick(table, hot_p[:, at], rankm_p[0:SOON, at], SOON),
                    pick(table_b, hot_p[:, at], rankm_p[SOON:CAP, at], CAP - SOON),
                )
            ]
        )
    amplitudes(
        soon_blocks, PTS // BLK, [jnp.concatenate([row[f] for row in found], axis=1) for f in range(FIELDS)]
    )
    green(SOON_PTS, PTS, False, True)

    slot = slot_ref[...]
    col_iota = lax.broadcasted_iota(jnp.int32, (DEV, NOBS), 0) * 2
    pieces = split3(sums[...])
    placed = []
    for parity in range(2):
        choose = jnp.where(col_iota + parity == slot, 1.0, 0.0).astype(BF16)
        placed.append(dot_nt(choose, pieces[0]) + dot_nt(choose, pieces[1]) + dot_nt(choose, pieces[2]))
    red_out[:, 0, :] = jnp.concatenate(placed, axis=1)
    exchange(red_out, red_in, 2, own=True)
    red_in[0] = red_out[me]
    cos_f, sin_f = sincos_twice(phase_ref[...] * 0.5)
    for blk in range(PTS // BLK):
        at = slice(blk * BLK, (blk + 1) * BLK)
        one = pick(table, hot[:, at], rankm[0:SOON, at], SOON)
        two = pick(table_b, hot[:, at], rankm[SOON:CAP, at], CAP - SOON)
        for f in range(FIELDS):
            surf_ref[f : f + 1, at] = one[f] + two[f]
    whole(red_in, 2).wait_recv()
    total = jnp.sum(red_in[:, 0, :], axis=0, keepdims=True)
    for parity in range(2):
        cosine = total[:, parity * 64 : parity * 64 + 32]
        sine = total[:, parity * 64 + 32 : parity * 64 + 64]
        spec_ref[0, parity : parity + 1, :] = prior_ref[0, parity : parity + 1, :] + (
            cos_f * cosine - sin_f * sine
        )
        spec_ref[1, parity : parity + 1, :] = prior_ref[1, parity : parity + 1, :] - (
            sin_f * cosine + cos_f * sine
        )
    whole(req_in, 0).wait_send()
    whole(rep_in, 1).wait_send()
    whole(rep_in_b, 3).wait_send()
    whole(red_in, 2).wait_send()


def on_device(
    element_fields,
    ref_coords,
    local_element,
    owner,
    point_angle,
    point_axial,
    panel_weight,
    obs_radius,
    obs_angle,
    obs_axial,
    step_phase,
    observer_slot,
    prior_spectra,
):
    vmem = pl.BlockSpec(memory_space=pltpu.VMEM)
    surface, spectra = pl.pallas_call(
        kernel,
        out_shape=(
            jax.ShapeDtypeStruct((FIELDS, PTS), F32),
            jax.ShapeDtypeStruct((2, 2, NFREQ), F32),
        ),
        in_specs=[pl.BlockSpec(memory_space=pltpu.HBM)] + [vmem] * 12,
        out_specs=(vmem, vmem),
        scratch_shapes=[
            pltpu.VMEM((FIELDS, ELEM, NODES), BF16),
            pltpu.VMEM((FIELDS * NODES, ELEM), BF16),
            pltpu.VMEM((2 * DEV, PTS), BF16),
            pltpu.VMEM((CAP, PTS), F32),
            pltpu.VMEM((DEV, 2, 128), F32),
            pltpu.VMEM((DEV, 2, 128), F32),
            pltpu.VMEM((CAP, 128), F32),
            pltpu.VMEM((CAP, 24, 128), F32),
            pltpu.VMEM((256, 128), F32),
            pltpu.VMEM((128, 128), F32),
            pltpu.VMEM((DEV, 2, 128), F32),
            pltpu.VMEM((DEV, 2, 128), F32),
            pltpu.VMEM((DEV, 1, 128), F32),
            pltpu.VMEM((DEV, 1, 128), F32),
            pltpu.VMEM((PTS - SOON_PTS, PTS), BF16),
            pltpu.VMEM((2 * DEV, PTS), BF16),
            pltpu.VMEM((CAP, PTS), F32),
            pltpu.VMEM((2, 66, 8, 128), F32),
            pltpu.VMEM((PTS, NOBS), F32),
            pltpu.VMEM((PTS // 8, 2, 8, 128), F32),
            pltpu.VMEM((PTS // 8, 2, 15, 8, 128), F32),
            pltpu.VMEM((2 * NFREQ, NOBS), F32),
            pltpu.VMEM((DEV, 1, 128), F32),
            pltpu.VMEM((DEV, 1, 128), F32),
            pltpu.SemaphoreType.DMA,
            pltpu.SemaphoreType.DMA((8,)),
        ],
        compiler_params=pltpu.CompilerParams(
            collective_id=0, has_side_effects=True, vmem_limit_bytes=63 * 1024 * 1024
        ),
        name="flow",
    )(
        element_fields.transpose(1, 0, 2),
        ref_coords,
        local_element.reshape(1, PTS),
        owner.reshape(1, PTS),
        point_angle.reshape(1, PTS),
        point_axial.reshape(1, PTS),
        panel_weight.reshape(1, PTS),
        obs_radius.reshape(1, NOBS),
        obs_angle.reshape(1, NOBS),
        obs_axial.reshape(1, NOBS),
        step_phase.reshape(1, NFREQ),
        observer_slot.reshape(1, NOBS),
        prior_spectra.transpose(0, 2, 1),
    )
    return surface, spectra.transpose(0, 2, 1)


def solution(mesh):
    return jax.shard_map(
        on_device,
        mesh=mesh,
        in_specs=(
            P(("gx", "gy"), None, None),
            P(None, ("gx", "gy")),
            P(("gx", "gy")),
            P(("gx", "gy"), None),
            P(("gx", "gy")),
            P(("gx", "gy")),
            P(("gx", "gy")),
            P(),
            P(),
            P(),
            P(),
            P(),
            P(None, None, ("gx", "gy")),
        ),
        out_specs=(P(None, ("gx", "gy")), P(None, None, ("gx", "gy"))),
        check_vma=False,
    )
```

```python
import math

import jax
import jax.numpy as jnp
import numpy as np
from jax import lax
from jax.experimental import pallas as pl
from jax.experimental.pallas import tpu as pltpu
from jax.sharding import PartitionSpec as P

LOGICAL = pl.DeviceIdType.LOGICAL
F32 = jnp.float32
BF16 = jnp.bfloat16

DEV = 128
INNER = 32
CAP = 64
PTS = 2048
ELEM = 512
NODES = 512
FIELDS = 5
NOBS = 256
NFREQ = 32
BLK = 256
WIDE = 8
UNROLL = 16
EVERY = 1
INSIDE = PTS // 8 - (20 // EVERY) * (CAP // WIDE)
SOON = 48
SOON_PTS = PTS * SOON // CAP
DELTAS = sorted(
    [(a, b, c, d) for a in range(4) for b in range(4) for c in range(4) for d in range(2)][1:],
    key=lambda t: -sum(min(v, 4 - v) for v in t[:3]) - 0.3 * t[3],
)

GLL = [
    -1.0,
    -0.8717401485096066,
    -0.5917001814331423,
    -0.2092992179024789,
    0.2092992179024789,
    0.5917001814331423,
    0.8717401485096066,
    1.0,
]
CENTRES = ((3, 2), (10, 4), (19, 4), (28, 4))


def fit_sincos():
    r = np.cos((np.arange(400) + 0.5) * np.pi / 400) * (np.pi / 2)
    x = r * r
    cheb = np.polynomial.chebyshev
    top = (np.pi / 2) ** 2

    def poly(y, degree):
        fitted = cheb.Chebyshev.fit(x, y, degree, domain=[0, top])
        return [float(v) for v in fitted.convert(kind=np.polynomial.Polynomial).coef]

    return poly(np.sin(r) / r, 5), poly(np.cos(r), 5)


SIN_C, COS_C = fit_sincos()
PI_HI = 3.140625
PI_LO = math.pi - 3.140625


def horner(coefs, x):
    total = coefs[-1] * x + coefs[-2]
    for value in coefs[-3::-1]:
        total = total * x + value
    return total


def sincos_twice(r):
    x = r * r
    s = horner(SIN_C, x) * r
    c = horner(COS_C, x)
    t = s + s
    return 1.0 - t * s, t * c


def lagrange(coord):
    gaps = [coord - node for node in GLL]
    left = [None, gaps[0]]
    for i in range(2, 8):
        left.append(left[-1] * gaps[i - 1])
    right = [None] * 8
    right[6] = gaps[7]
    for i in range(5, -1, -1):
        right[i] = right[i + 1] * gaps[i + 1]
    values = []
    for i in range(8):
        divisor = 1.0
        for m in range(8):
            if m != i:
                divisor *= GLL[i] - GLL[m]
        scale = float(1.0 / divisor)
        if i == 0:
            product = right[0]
        elif i == 7:
            product = left[7]
        else:
            product = left[i] * right[i]
        values.append(product * scale)
    return values


def split2(x):
    hi = x.astype(BF16)
    lo = (x - hi.astype(F32)).astype(BF16)
    return hi, lo


def split3(x):
    hi = x.astype(BF16)
    rest = x - hi.astype(F32)
    mid = rest.astype(BF16)
    lo = (rest - mid.astype(F32)).astype(BF16)
    return hi, mid, lo


def products(left, right, mine, theirs):
    a = [piece.astype(F32) for piece in split3(mine)]
    b = [piece.astype(F32) for piece in split3(theirs)]
    for i in range(3):
        for j in range(3 - i):
            left.append(a[i])
            right.append(b[j])


def dot_nt(a, b):
    return lax.dot_general(a, b, (((1,), (1,)), ((), ())), preferred_element_type=F32)


def dot_nn(a, b):
    return lax.dot_general(a, b, (((1,), (0,)), ((), ())), preferred_element_type=F32)


def kernel(
    tab_hbm,
    coords_ref,
    local_ref,
    owner_ref,
    angle_ref,
    axial_ref,
    weight_ref,
    orad_ref,
    oang_ref,
    oax_ref,
    phase_ref,
    slot_ref,
    prior_ref,
    surf_ref,
    spec_ref,
    tab,
    tabt,
    hot,
    rankm,
    req_out,
    req_in,
    rid,
    lag,
    lag_t,
    valt,
    valt_b,
    rep_out,
    rep_in,
    rep_out_b,
    rep_in_b,
    swap,
    hot_p,
    rankm_p,
    partial,
    square_ref,
    amp,
    geo,
    sums,
    red_out,
    red_in,
    tab_sem,
    sems,
):
    me = lax.axis_index("gx") * INNER + lax.axis_index("gy")

    y, x, z, core = me // 32, lax.rem(me // 8, 4), lax.rem(me // 2, 4), lax.rem(me, 2)

    def target(delta):
        dy, dx, dz, dc = delta
        return (
            lax.rem(y + dy, 4) * 32 + lax.rem(x + dx, 4) * 8 + lax.rem(z + dz, 4) * 2 + lax.rem(core + dc, 2)
        )

    def others(body):
        for delta in DELTAS:
            code = delta[0] * 32 + delta[1] * 8 + delta[2] * 2 + delta[3]
            body(code, target(delta), target(((4 - delta[0]) % 4, (4 - delta[1]) % 4, (4 - delta[2]) % 4, delta[3])))

    tab_copy = pltpu.make_async_copy(tab_hbm, tab, tab_sem)
    tab_copy.start()
    barrier = pltpu.get_barrier_semaphore()
    others(
        lambda code, there, back: pl.semaphore_signal(
            barrier, inc=1, device_id=there, device_id_type=LOGICAL
        )
    )

    def exchange(source, landing, k, own=False, reply=False):
        def send(code, there, back):
            pltpu.make_async_remote_copy(
                src_ref=source.at[there if own else code],
                dst_ref=landing.at[code],
                send_sem=sems.at[2 * k],
                recv_sem=sems.at[2 * k + 1],
                device_id=back if reply else there,
                device_id_type=LOGICAL,
            ).start()

        others(send)

    def whole(landing, k):
        rest = landing.at[pl.ds(1, DEV - 1)]
        return pltpu.make_async_remote_copy(
            src_ref=rest,
            dst_ref=rest,
            send_sem=sems.at[2 * k],
            recv_sem=sems.at[2 * k + 1],
            device_id=lax.rem(me + 1, DEV),
            device_id_type=LOGICAL,
        )

    own = owner_ref[...]
    rel = (
        ((own // 32 - y + 4) & 3) * 32
        + (((own // 8) & 3) - x + 4 & 3) * 8
        + (((own // 2) & 3) - z + 4 & 3) * 2
        + ((own & 1) - core + 2 & 1)
    )
    dev_iota = lax.broadcasted_iota(jnp.int32, (DEV, BLK), 0)
    cap_iota = lax.broadcasted_iota(jnp.int32, (CAP, BLK), 0)
    before = jnp.where(
        lax.broadcasted_iota(jnp.int32, (BLK, BLK), 0) < lax.broadcasted_iota(jnp.int32, (BLK, BLK), 1),
        1.0,
        0.0,
    ).astype(BF16)
    offset = jnp.zeros((DEV, 1), F32)
    packed = jnp.zeros((DEV, 4 * CAP), F32)
    swap_iota = lax.broadcasted_iota(jnp.int32, (PTS - SOON_PTS, BLK), 0)
    count = jnp.zeros((1, 1), F32)
    wrong = None
    ranks, swaps = [], []
    for blk in range(PTS // BLK):
        at = slice(blk * BLK, (blk + 1) * BLK)
        onehot = jnp.where(dev_iota == rel[:, at], 1.0, 0.0)
        onehot16 = onehot.astype(BF16)
        hot[0:DEV, at] = onehot16
        hot[DEV : 2 * DEV, at] = onehot16
        within = dot_nn(onehot16, before)
        rank = jnp.sum(onehot * (within + offset), axis=0, keepdims=True)
        offset = offset + jnp.sum(onehot, axis=1, keepdims=True)
        if blk * BLK == SOON_PTS:
            wrong = count
            count = jnp.zeros((1, 1), F32)
        flag = jnp.where(rank >= SOON if blk * BLK < SOON_PTS else rank < SOON, 1.0, 0.0)
        number = dot_nn(jnp.broadcast_to(flag, (8, BLK)).astype(BF16), before)[0:1] + count
        count = count + jnp.sum(flag, axis=1, keepdims=True)
        if wrong is not None:
            flag = jnp.where(number < wrong, flag, 0.0)
        number = jnp.where(flag > 0.5, number, -1.0).astype(jnp.int32)
        swap[:, at] = jnp.where(swap_iota == number, 1.0, 0.0).astype(BF16)
        ranks.append(rank)
        swaps.append(flag)
        mask = cap_iota == rank.astype(jnp.int32)
        rankm[:, at] = jnp.where(mask, 1.0, 0.0)
        rows = [local_ref[:, at].astype(F32)] + [coords_ref[v : v + 1, at] for v in range(3)]
        pieces = [split3(row) for row in rows]
        for part in range(3):
            table = jnp.concatenate(
                [jnp.where(mask, pieces[v][part].astype(F32), 0.0) for v in range(4)], axis=0
            ).astype(BF16)
            packed = packed + dot_nt(onehot16, table)
    req_out[:, 0, :] = packed[:, 0:128]
    req_out[:, 1, :] = packed[:, 128:256]

    cos_p, sin_p = sincos_twice(angle_ref[...] * 0.5)
    attributes = [piece.astype(F32) for row in (cos_p, sin_p, axial_ref[...], weight_ref[...]) for piece in split3(row)]
    attributes.append(rel.astype(F32))
    attributes.append(jnp.concatenate(ranks, axis=1))
    attributes.append(jnp.zeros((2, PTS), F32))
    attributes = jnp.concatenate(attributes, axis=0).astype(BF16)
    to_first = dot_nt(attributes[:, SOON_PTS:], swap[:, SOON_PTS:]).astype(BF16)
    to_last = dot_nt(attributes[:, :SOON_PTS], swap[:, :SOON_PTS]).astype(BF16)
    moved = jnp.concatenate(
        [dot_nn(to_first, swap[:, :SOON_PTS]), dot_nn(to_last, swap[:, SOON_PTS:])], axis=1
    )
    ordered = jnp.where(jnp.concatenate(swaps, axis=1) > 0.5, moved, attributes.astype(F32))
    cos_p, sin_p, axial, panel = [
        ordered[n : n + 1] + ordered[n + 1 : n + 2] + ordered[n + 2 : n + 3] for n in (0, 3, 6, 9)
    ]
    rel_p = ordered[12:13].astype(jnp.int32)
    rank_p = ordered[13:14].astype(jnp.int32)
    for blk in range(PTS // BLK):
        at = slice(blk * BLK, (blk + 1) * BLK)
        onehot16 = jnp.where(dev_iota == rel_p[:, at], 1.0, 0.0).astype(BF16)
        hot_p[0:DEV, at] = onehot16
        hot_p[DEV : 2 * DEV, at] = onehot16
        rankm_p[:, at] = jnp.where(cap_iota == rank_p[:, at], 1.0, 0.0)

    pl.semaphore_wait(barrier, DEV - 1)
    exchange(req_out, req_in, 0)
    req_in[0] = req_out[0]

    cos_o, sin_o = sincos_twice(oang_ref[...] * 0.5)
    orad = orad_ref[...]
    obs_x = orad * cos_o
    obs_y = orad * sin_o
    obs_z = oax_ref[...]
    mid_p = axial - 4.0
    mid_o = obs_z - 4.0
    left, right = [], []
    for mine, theirs in ((cos_p * -2.0, obs_x), (sin_p * -2.0, obs_y), (mid_p * -2.0, mid_o)):
        products(left, right, mine, theirs)
    one_p = jnp.ones((1, PTS), F32)
    one_o = jnp.ones((1, NOBS), F32)
    for piece in split3(mid_p * mid_p + 1.0):
        left.append(piece.astype(F32))
        right.append(one_o)
    for piece in split3(orad * orad + mid_o * mid_o):
        left.append(one_p)
        right.append(piece.astype(F32))
    square_ref[...] = dot_nn(jnp.concatenate(left, axis=0).T.astype(BF16), jnp.concatenate(right, axis=0).astype(BF16))
    tab_copy.wait()
    for f in range(FIELDS):
        tabt[f * NODES : (f + 1) * NODES, :] = tab[f].T

    def geometry(first, last):
        @pl.loop(first, last)
        def _(step):
            pairs_of([(step * 2 + u, g) for u in range(2) for g in range(2)])

    def pairs_of(places):
        if True:
            if True:
                for blk, g in places:
                    square = square_ref[pl.ds(pl.multiple_of(blk * 8, 8), 8), g * 128 : (g + 1) * 128]
                    inv = lax.rsqrt(square)
                    dist = square * inv
                    turns = jnp.round(dist * (0.125 / math.pi))
                    r = dist * 0.125 - turns * PI_HI - turns * PI_LO
                    c1, s1 = sincos_twice(r)
                    t = c1 + c1
                    c2 = t * c1 - 1.0
                    s2 = t * s1
                    c3 = t * c2 - c1
                    s3 = t * s2 - s1
                    c4 = t * c3 - c2
                    s4 = t * s3 - s2
                    c5 = t * c4 - c3
                    s5 = t * s4 - s3
                    t5 = c5 + c5
                    c10 = t5 * c5 - 1.0
                    s10 = t5 * s5
                    c9 = t5 * c4 - c1
                    t9 = c9 + c9
                    c19 = t9 * c10 - c1
                    s19 = t9 * s10 - s1
                    c28 = t9 * c19 - c10
                    s28 = t9 * s19 - s10
                    for n, value in enumerate(
                        (c1, s1, c2, s2, c3, s3, c4, s4, c10, s10, c19, s19, c28, s28, inv)
                    ):
                        geo[blk, g, n] = value

    geometry(0, INSIDE // 2)

    whole(req_in, 0).wait_recv()

    first = req_in[:, 0, :].T
    second = req_in[:, 1, :].T
    rid[...] = first[0:CAP]
    for n, value in enumerate((first[CAP : 2 * CAP], second[0:CAP])):
        for i, weight in enumerate(lagrange(value)):
            lag[n * 8 + i] = weight
    for i, weight in enumerate(lagrange(second[CAP : 2 * CAP])):
        lag_t[:, i, :] = weight

    elem_iota = lax.broadcasted_iota(jnp.int32, (ELEM, 128), 0).astype(F32)

    def gather(group, land, first, span):
        picks = []
        weights = []
        inner_weights = []
        for part in range(WIDE):
            c = group * WIDE + part
            picks.append(jnp.where(elem_iota == rid[pl.ds(c, 1), :], 1.0, 0.0).astype(BF16))
            weights.append([lag[n, pl.ds(c, 1), :] for n in range(16)])
            inner_weights.append(lag_t[c])
        pick = jnp.concatenate(picks, axis=1)
        weight = [jnp.concatenate([row[n] for row in weights], axis=1) for n in range(16)]
        inner_weight = jnp.concatenate(inner_weights, axis=1)
        for f in range(FIELDS):
            nodal = dot_nn(tabt[f * NODES : (f + 1) * NODES, :], pick)
            total = None
            for i in range(8):
                inner = None
                for j in range(8):
                    at = (i * 8 + j) * 8
                    term = nodal[at : at + 8, :] * weight[8 + j]
                    inner = term if inner is None else inner + term
                inner = inner * weight[i]
                total = inner if total is None else total + inner
                if i % EVERY == 0:
                    unit = f * (8 // EVERY) + i // EVERY
                    pairs_of([(INSIDE + group * (20 // EVERY) + unit // 2, unit % 2)])
            value = jnp.sum(total * inner_weight, axis=0, keepdims=True)
            for part in range(WIDE):
                land[pl.ds(f * span + (group * WIDE - first) + part, 1), :] = value[:, part * 128 : (part + 1) * 128]

    pl.loop(0, SOON // WIDE)(lambda group: gather(group, valt, 0, SOON))
    valt[FIELDS * SOON : 256, :] = jnp.zeros((256 - FIELDS * SOON, 128), F32)
    for n in range(2):
        rep_out[:, n, :] = valt[n * 128 : (n + 1) * 128, :].T
    exchange(rep_out, rep_in, 1, reply=True)
    rep_in[0] = rep_out[0]
    pl.loop(SOON // WIDE, CAP // WIDE)(lambda group: gather(group, valt_b, SOON, CAP - SOON))
    valt_b[FIELDS * (CAP - SOON) : 128, :] = jnp.zeros((128 - FIELDS * (CAP - SOON), 128), F32)
    rep_out_b[:, 0, :] = valt_b[...].T
    exchange(rep_out_b, rep_in_b, 3, reply=True)
    rep_in_b[0] = rep_out_b[0]

    def sources(landing, count):
        parts = [split2(landing[:, n, :].T) for n in range(count)]
        return jnp.concatenate(
            [
                jnp.concatenate([hi for hi, lo in parts], axis=0),
                jnp.concatenate([lo for hi, lo in parts], axis=0),
            ],
            axis=1,
        )

    def pick(table, choose, mask, span):
        found = dot_nn(table, choose)
        return [
            jnp.sum(found[f * span : (f + 1) * span, :] * mask, axis=0, keepdims=True) for f in range(FIELDS)
        ]

    def amplitudes(first, last, values):
        at_p = slice(first * BLK, last * BLK)
        density, vel_x, vel_y, vel_z, pressure = values
        cos_q, sin_q, axial_q = cos_p[:, at_p], sin_p[:, at_p], axial[:, at_p]
        normal = vel_x * cos_q + vel_y * sin_q
        scaled = panel[:, at_p] * (1.0 / math.sqrt(PTS * DEV))
        flux = density * normal * scaled
        pressure = pressure * scaled
        left, right = [], []
        products(left, right, pressure * cos_q + flux * vel_x, obs_x)
        products(left, right, pressure * sin_q + flux * vel_y, obs_y)
        products(left, right, flux * vel_z, obs_z)
        for piece in split3(-(pressure + flux * (normal + vel_z * axial_q))):
            left.append(piece.astype(F32))
            right.append(one_o)
        zero_o = jnp.zeros((1, NOBS), F32)
        other = [zero_o] * len(left)
        for piece in split3(flux):
            left.append(piece.astype(F32))
            right.append(zero_o)
            other.append(one_o)
        left = jnp.concatenate(left, axis=0).T.astype(BF16)
        right = jnp.concatenate(
            [jnp.concatenate(right, axis=0), jnp.concatenate(other, axis=0)], axis=1
        ).astype(BF16)
        for blk in range(last - first):
            mixed = dot_nn(left[blk * BLK : (blk + 1) * BLK, :], right)
            for n in range(BLK // 8):
                at = (first + blk) * (BLK // 8) + n
                for g in range(2):
                    lanes = slice(g * 128, (g + 1) * 128)
                    inv = geo[at, g, 14]
                    linear = mixed[n * 8 : n * 8 + 8, lanes]
                    amp[at, g] = (
                        mixed[n * 8 : n * 8 + 8, 256 + g * 128 : 384 + g * 128] + linear * inv
                    ) * (inv * orad[:, lanes])

    def put(k, lanes, cosine, sine):
        sums[k - 1 : k, lanes] = jnp.sum(cosine, axis=0, keepdims=True)
        sums[NFREQ + k - 1 : NFREQ + k, lanes] = jnp.sum(sine, axis=0, keepdims=True)

    def green(first, last, begin, end):
        for g in range(2):
            lanes = slice(g * 128, (g + 1) * 128)
            base = 0
            for number, (centre, reach) in enumerate(CENTRES):

                def body(step, acc, number=number, reach=reach, g=g):
                    acc = list(acc)
                    for u in range(UNROLL):
                        blk = step * UNROLL + u
                        a = amp[blk, g]
                        at = 4 if number == 0 else 6 + 2 * number
                        ac = a * geo[blk, g, at]
                        as_ = a * geo[blk, g, at + 1]
                        acc[0] = acc[0] + ac
                        acc[1] = acc[1] + as_
                        for b in range(reach):
                            yc = geo[blk, g, 2 * b]
                            ysn = geo[blk, g, 2 * b + 1]
                            acc[2 + 4 * b] = acc[2 + 4 * b] + ac * yc
                            acc[3 + 4 * b] = acc[3 + 4 * b] + as_ * ysn
                            acc[4 + 4 * b] = acc[4 + 4 * b] + as_ * yc
                            acc[5 + 4 * b] = acc[5 + 4 * b] + ac * ysn
                    return tuple(acc)

                count = 2 + 4 * reach
                if begin:
                    start = tuple(jnp.zeros((8, 128), F32) for _ in range(count))
                else:
                    start = tuple(partial[g, base + n] for n in range(count))
                acc = lax.fori_loop(first // (8 * UNROLL), last // (8 * UNROLL), body, start)
                if end:
                    put(centre, lanes, acc[0], acc[1])
                    for b in range(reach):
                        p1, p2, p3, p4 = acc[2 + 4 * b : 6 + 4 * b]
                        put(centre + b + 1, lanes, p1 - p2, p3 + p4)
                        put(centre - b - 1, lanes, p1 + p2, p3 - p4)
                else:
                    for n in range(count):
                        partial[g, base + n] = acc[n]
                base += count

    whole(rep_in, 1).wait_recv()
    table = sources(rep_in, 2)
    soon_blocks = SOON_PTS // BLK
    found = []
    for blk in range(soon_blocks):
        at = slice(blk * BLK, (blk + 1) * BLK)
        found.append(pick(table, hot_p[:, at], rankm_p[0:SOON, at], SOON))
    amplitudes(0, soon_blocks, [jnp.concatenate([row[f] for row in found], axis=1) for f in range(FIELDS)])
    green(0, SOON_PTS, True, False)
    whole(rep_in_b, 3).wait_recv()
    table_b = sources(rep_in_b, 1)
    found = []
    for blk in range(soon_blocks, PTS // BLK):
        at = slice(blk * BLK, (blk + 1) * BLK)
        found.append(
            [
                one + two
                for one, two in zip(
                    pick(table, hot_p[:, at], rankm_p[0:SOON, at], SOON),
                    pick(table_b, hot_p[:, at], rankm_p[SOON:CAP, at], CAP - SOON),
                )
            ]
        )
    amplitudes(
        soon_blocks, PTS // BLK, [jnp.concatenate([row[f] for row in found], axis=1) for f in range(FIELDS)]
    )
    green(SOON_PTS, PTS, False, True)

    slot = slot_ref[...]
    col_iota = lax.broadcasted_iota(jnp.int32, (DEV, NOBS), 0) * 2
    pieces = split3(sums[...])
    placed = []
    for parity in range(2):
        choose = jnp.where(col_iota + parity == slot, 1.0, 0.0).astype(BF16)
        placed.append(dot_nt(choose, pieces[0]) + dot_nt(choose, pieces[1]) + dot_nt(choose, pieces[2]))
    red_out[:, 0, :] = jnp.concatenate(placed, axis=1)
    exchange(red_out, red_in, 2, own=True)
    red_in[0] = red_out[me]
    cos_f, sin_f = sincos_twice(phase_ref[...] * 0.5)
    for blk in range(PTS // BLK):
        at = slice(blk * BLK, (blk + 1) * BLK)
        one = pick(table, hot[:, at], rankm[0:SOON, at], SOON)
        two = pick(table_b, hot[:, at], rankm[SOON:CAP, at], CAP - SOON)
        for f in range(FIELDS):
            surf_ref[f : f + 1, at] = one[f] + two[f]
    whole(red_in, 2).wait_recv()
    total = jnp.sum(red_in[:, 0, :], axis=0, keepdims=True)
    for parity in range(2):
        cosine = total[:, parity * 64 : parity * 64 + 32]
        sine = total[:, parity * 64 + 32 : parity * 64 + 64]
        spec_ref[0, parity : parity + 1, :] = prior_ref[0, parity : parity + 1, :] + (
            cos_f * cosine - sin_f * sine
        )
        spec_ref[1, parity : parity + 1, :] = prior_ref[1, parity : parity + 1, :] - (
            sin_f * cosine + cos_f * sine
        )
    whole(req_in, 0).wait_send()
    whole(rep_in, 1).wait_send()
    whole(rep_in_b, 3).wait_send()
    whole(red_in, 2).wait_send()


def hand_over(surface_in, spectra_in, surface_out, spectra_out, sems):
    copies = [
        pltpu.make_async_copy(surface_in, surface_out, sems.at[0]),
        pltpu.make_async_copy(spectra_in, spectra_out, sems.at[1]),
    ]
    for copy in copies:
        copy.start()
    for copy in copies:
        copy.wait()


def on_device(
    element_fields,
    ref_coords,
    local_element,
    owner,
    point_angle,
    point_axial,
    panel_weight,
    obs_radius,
    obs_angle,
    obs_axial,
    step_phase,
    observer_slot,
    prior_spectra,
):
    vmem = pl.BlockSpec(memory_space=pltpu.VMEM)
    surface, spectra = pl.pallas_call(
        kernel,
        out_shape=(pltpu.VMEM((FIELDS, PTS), F32), pltpu.VMEM((2, 2, NFREQ), F32)),
        in_specs=[pl.BlockSpec(memory_space=pltpu.HBM)] + [vmem] * 12,
        out_specs=(vmem, vmem),
        scratch_shapes=[
            pltpu.VMEM((FIELDS, ELEM, NODES), BF16),
            pltpu.VMEM((FIELDS * NODES, ELEM), BF16),
            pltpu.VMEM((2 * DEV, PTS), BF16),
            pltpu.VMEM((CAP, PTS), F32),
            pltpu.VMEM((DEV, 2, 128), F32),
            pltpu.VMEM((DEV, 2, 128), F32),
            pltpu.VMEM((CAP, 128), F32),
            pltpu.VMEM((16, CAP, 128), F32),
            pltpu.VMEM((CAP, 8, 128), F32),
            pltpu.VMEM((256, 128), F32),
            pltpu.VMEM((128, 128), F32),
            pltpu.VMEM((DEV, 2, 128), F32),
            pltpu.VMEM((DEV, 2, 128), F32),
            pltpu.VMEM((DEV, 1, 128), F32),
            pltpu.VMEM((DEV, 1, 128), F32),
            pltpu.VMEM((PTS - SOON_PTS, PTS), BF16),
            pltpu.VMEM((2 * DEV, PTS), BF16),
            pltpu.VMEM((CAP, PTS), F32),
            pltpu.VMEM((2, 66, 8, 128), F32),
            pltpu.VMEM((PTS, NOBS), F32),
            pltpu.VMEM((PTS // 8, 2, 8, 128), F32),
            pltpu.VMEM((PTS // 8, 2, 15, 8, 128), F32),
            pltpu.VMEM((2 * NFREQ, NOBS), F32),
            pltpu.VMEM((DEV, 1, 128), F32),
            pltpu.VMEM((DEV, 1, 128), F32),
            pltpu.SemaphoreType.DMA,
            pltpu.SemaphoreType.DMA((8,)),
        ],
        compiler_params=pltpu.CompilerParams(
            collective_id=0, has_side_effects=True, vmem_limit_bytes=63 * 1024 * 1024
        ),
        name="flow",
    )(
        element_fields.transpose(1, 0, 2),
        ref_coords,
        local_element.reshape(1, PTS),
        owner.reshape(1, PTS),
        point_angle.reshape(1, PTS),
        point_axial.reshape(1, PTS),
        panel_weight.reshape(1, PTS),
        obs_radius.reshape(1, NOBS),
        obs_angle.reshape(1, NOBS),
        obs_axial.reshape(1, NOBS),
        step_phase.reshape(1, NFREQ),
        observer_slot.reshape(1, NOBS),
        prior_spectra.transpose(0, 2, 1),
    )
    surface, spectra = pl.pallas_call(
        hand_over,
        out_shape=(
            jax.ShapeDtypeStruct((FIELDS, PTS), F32),
            jax.ShapeDtypeStruct((2, 2, NFREQ), F32),
        ),
        in_specs=[vmem, vmem],
        out_specs=(pl.BlockSpec(memory_space=pltpu.HBM), pl.BlockSpec(memory_space=pltpu.HBM)),
        scratch_shapes=[pltpu.SemaphoreType.DMA((2,))],
        name="hand_over",
    )(
        pltpu.with_memory_space_constraint(surface, pltpu.VMEM),
        pltpu.with_memory_space_constraint(spectra, pltpu.VMEM),
    )
    return surface, spectra.transpose(0, 2, 1)


def solution(mesh):
    return jax.shard_map(
        on_device,
        mesh=mesh,
        in_specs=(
            P(("gx", "gy"), None, None),
            P(None, ("gx", "gy")),
            P(("gx", "gy")),
            P(("gx", "gy"), None),
            P(("gx", "gy")),
            P(("gx", "gy")),
            P(("gx", "gy")),
            P(),
            P(),
            P(),
            P(),
            P(),
            P(None, None, ("gx", "gy")),
        ),
        out_specs=(P(None, ("gx", "gy")), P(None, None, ("gx", "gy"))),
        check_vma=False,
    )
```

```python
import math

import jax
import jax.numpy as jnp
import numpy as np
from jax import lax
from jax.experimental import pallas as pl
from jax.experimental.pallas import tpu as pltpu
from jax.sharding import PartitionSpec as P

LOGICAL = pl.DeviceIdType.LOGICAL
F32 = jnp.float32
BF16 = jnp.bfloat16

DEV = 128
INNER = 32
CAP = 64
PTS = 2048
ELEM = 512
NODES = 512
FIELDS = 5
NOBS = 256
NFREQ = 32
BLK = 256
WIDE = 8
UNROLL = 16
EVERY = 1
INSIDE = PTS // 8 - (20 // EVERY) * (CAP // WIDE)
SOON = 48
SOON_PTS = PTS * SOON // CAP
DELTAS = sorted(
    [(a, b, c, d) for a in range(4) for b in range(4) for c in range(4) for d in range(2)][1:],
    key=lambda t: -sum(min(v, 4 - v) for v in t[:3]) - 0.3 * t[3],
)

GLL = [
    -1.0,
    -0.8717401485096066,
    -0.5917001814331423,
    -0.2092992179024789,
    0.2092992179024789,
    0.5917001814331423,
    0.8717401485096066,
    1.0,
]
CENTRES = ((3, 2), (10, 4), (19, 4), (28, 4))


def fit_sincos():
    r = np.cos((np.arange(400) + 0.5) * np.pi / 400) * (np.pi / 2)
    x = r * r
    cheb = np.polynomial.chebyshev
    top = (np.pi / 2) ** 2

    def poly(y, degree):
        fitted = cheb.Chebyshev.fit(x, y, degree, domain=[0, top])
        return [float(v) for v in fitted.convert(kind=np.polynomial.Polynomial).coef]

    return poly(np.sin(r) / r, 5), poly(np.cos(r), 5)


SIN_C, COS_C = fit_sincos()
PI_HI = 3.140625
PI_LO = math.pi - 3.140625


def horner(coefs, x):
    total = coefs[-1] * x + coefs[-2]
    for value in coefs[-3::-1]:
        total = total * x + value
    return total


def sincos_twice(r):
    x = r * r
    s = horner(SIN_C, x) * r
    c = horner(COS_C, x)
    t = s + s
    return 1.0 - t * s, t * c


def lagrange(coord):
    gaps = [coord - node for node in GLL]
    left = [None, gaps[0]]
    for i in range(2, 8):
        left.append(left[-1] * gaps[i - 1])
    right = [None] * 8
    right[6] = gaps[7]
    for i in range(5, -1, -1):
        right[i] = right[i + 1] * gaps[i + 1]
    values = []
    for i in range(8):
        divisor = 1.0
        for m in range(8):
            if m != i:
                divisor *= GLL[i] - GLL[m]
        scale = float(1.0 / divisor)
        if i == 0:
            product = right[0]
        elif i == 7:
            product = left[7]
        else:
            product = left[i] * right[i]
        values.append(product * scale)
    return values


def split2(x):
    hi = x.astype(BF16)
    lo = (x - hi.astype(F32)).astype(BF16)
    return hi, lo


def split3(x):
    hi = x.astype(BF16)
    rest = x - hi.astype(F32)
    mid = rest.astype(BF16)
    lo = (rest - mid.astype(F32)).astype(BF16)
    return hi, mid, lo


def products(left, right, mine, theirs):
    a = [piece.astype(F32) for piece in split3(mine)]
    b = [piece.astype(F32) for piece in split3(theirs)]
    for i in range(3):
        for j in range(3 - i):
            left.append(a[i])
            right.append(b[j])


def dot_nt(a, b):
    return lax.dot_general(a, b, (((1,), (1,)), ((), ())), preferred_element_type=F32)


def dot_nn(a, b):
    return lax.dot_general(a, b, (((1,), (0,)), ((), ())), preferred_element_type=F32)


def kernel(
    tab_hbm,
    coords_ref,
    local_ref,
    owner_ref,
    angle_ref,
    axial_ref,
    weight_ref,
    orad_ref,
    oang_ref,
    oax_ref,
    phase_ref,
    slot_ref,
    prior_ref,
    surf_ref,
    spec_ref,
    tab,
    tabt,
    hot,
    rankm,
    req_out,
    req_in,
    rid,
    lag,
    lag_t,
    valt,
    valt_b,
    rep_out,
    rep_in,
    rep_out_b,
    rep_in_b,
    swap,
    hot_p,
    rankm_p,
    partial,
    square_ref,
    amp,
    geo,
    sums,
    red_out,
    red_in,
    tab_sem,
    sems,
):
    me = lax.axis_index("gx") * INNER + lax.axis_index("gy")

    y, x, z, core = me // 32, lax.rem(me // 8, 4), lax.rem(me // 2, 4), lax.rem(me, 2)

    def target(delta):
        dy, dx, dz, dc = delta
        return (
            lax.rem(y + dy, 4) * 32 + lax.rem(x + dx, 4) * 8 + lax.rem(z + dz, 4) * 2 + lax.rem(core + dc, 2)
        )

    def others(body):
        for delta in DELTAS:
            code = delta[0] * 32 + delta[1] * 8 + delta[2] * 2 + delta[3]
            body(code, target(delta), target(((4 - delta[0]) % 4, (4 - delta[1]) % 4, (4 - delta[2]) % 4, delta[3])))

    tab_copy = pltpu.make_async_copy(tab_hbm, tab, tab_sem)
    tab_copy.start()
    barrier = pltpu.get_barrier_semaphore()
    others(
        lambda code, there, back: pl.semaphore_signal(
            barrier, inc=1, device_id=there, device_id_type=LOGICAL
        )
    )

    def exchange(source, landing, k, own=False, reply=False):
        def send(code, there, back):
            pltpu.make_async_remote_copy(
                src_ref=source.at[there if own else code],
                dst_ref=landing.at[code],
                send_sem=sems.at[2 * k],
                recv_sem=sems.at[2 * k + 1],
                device_id=back if reply else there,
                device_id_type=LOGICAL,
            ).start()

        others(send)

    def whole(landing, k):
        rest = landing.at[pl.ds(1, DEV - 1)]
        return pltpu.make_async_remote_copy(
            src_ref=rest,
            dst_ref=rest,
            send_sem=sems.at[2 * k],
            recv_sem=sems.at[2 * k + 1],
            device_id=lax.rem(me + 1, DEV),
            device_id_type=LOGICAL,
        )

    own = owner_ref[...]
    rel = (
        ((own // 32 - y + 4) & 3) * 32
        + (((own // 8) & 3) - x + 4 & 3) * 8
        + (((own // 2) & 3) - z + 4 & 3) * 2
        + ((own & 1) - core + 2 & 1)
    )
    dev_iota = lax.broadcasted_iota(jnp.int32, (DEV, BLK), 0)
    cap_iota = lax.broadcasted_iota(jnp.int32, (CAP, BLK), 0)
    before = jnp.where(
        lax.broadcasted_iota(jnp.int32, (BLK, BLK), 0) < lax.broadcasted_iota(jnp.int32, (BLK, BLK), 1),
        1.0,
        0.0,
    ).astype(BF16)
    offset = jnp.zeros((DEV, 1), F32)
    packed = jnp.zeros((DEV, 4 * CAP), F32)
    swap_iota = lax.broadcasted_iota(jnp.int32, (PTS - SOON_PTS, BLK), 0)
    count = jnp.zeros((1, 1), F32)
    wrong = None
    ranks, swaps = [], []
    for blk in range(PTS // BLK):
        at = slice(blk * BLK, (blk + 1) * BLK)
        onehot = jnp.where(dev_iota == rel[:, at], 1.0, 0.0)
        onehot16 = onehot.astype(BF16)
        hot[0:DEV, at] = onehot16
        hot[DEV : 2 * DEV, at] = onehot16
        within = dot_nn(onehot16, before)
        rank = jnp.sum(onehot * (within + offset), axis=0, keepdims=True)
        offset = offset + jnp.sum(onehot, axis=1, keepdims=True)
        if blk * BLK == SOON_PTS:
            wrong = count
            count = jnp.zeros((1, 1), F32)
        flag = jnp.where(rank >= SOON if blk * BLK < SOON_PTS else rank < SOON, 1.0, 0.0)
        number = dot_nn(jnp.broadcast_to(flag, (8, BLK)).astype(BF16), before)[0:1] + count
        count = count + jnp.sum(flag, axis=1, keepdims=True)
        if wrong is not None:
            flag = jnp.where(number < wrong, flag, 0.0)
        number = jnp.where(flag > 0.5, number, -1.0).astype(jnp.int32)
        swap[:, at] = jnp.where(swap_iota == number, 1.0, 0.0).astype(BF16)
        ranks.append(rank)
        swaps.append(flag)
        mask = cap_iota == rank.astype(jnp.int32)
        rankm[:, at] = jnp.where(mask, 1.0, 0.0)
        rows = [local_ref[:, at].astype(F32)] + [coords_ref[v : v + 1, at] for v in range(3)]
        pieces = [split3(row) for row in rows]
        for part in range(3):
            table = jnp.concatenate(
                [jnp.where(mask, pieces[v][part].astype(F32), 0.0) for v in range(4)], axis=0
            ).astype(BF16)
            packed = packed + dot_nt(onehot16, table)
    req_out[:, 0, :] = packed[:, 0:128]
    req_out[:, 1, :] = packed[:, 128:256]

    pl.semaphore_wait(barrier, DEV - 1)
    exchange(req_out, req_in, 0)
    req_in[0] = req_out[0]

    cos_p, sin_p = sincos_twice(angle_ref[...] * 0.5)
    attributes = [piece.astype(F32) for row in (cos_p, sin_p, axial_ref[...], weight_ref[...]) for piece in split3(row)]
    attributes.append(rel.astype(F32))
    attributes.append(jnp.concatenate(ranks, axis=1))
    attributes.append(jnp.zeros((2, PTS), F32))
    attributes = jnp.concatenate(attributes, axis=0).astype(BF16)
    to_first = dot_nt(attributes[:, SOON_PTS:], swap[:, SOON_PTS:]).astype(BF16)
    to_last = dot_nt(attributes[:, :SOON_PTS], swap[:, :SOON_PTS]).astype(BF16)
    moved = jnp.concatenate(
        [dot_nn(to_first, swap[:, :SOON_PTS]), dot_nn(to_last, swap[:, SOON_PTS:])], axis=1
    )
    ordered = jnp.where(jnp.concatenate(swaps, axis=1) > 0.5, moved, attributes.astype(F32))
    cos_p, sin_p, axial, panel = [
        ordered[n : n + 1] + ordered[n + 1 : n + 2] + ordered[n + 2 : n + 3] for n in (0, 3, 6, 9)
    ]
    rel_p = ordered[12:13].astype(jnp.int32)
    rank_p = ordered[13:14].astype(jnp.int32)
    for blk in range(PTS // BLK):
        at = slice(blk * BLK, (blk + 1) * BLK)
        onehot16 = jnp.where(dev_iota == rel_p[:, at], 1.0, 0.0).astype(BF16)
        hot_p[0:DEV, at] = onehot16
        hot_p[DEV : 2 * DEV, at] = onehot16
        rankm_p[:, at] = jnp.where(cap_iota == rank_p[:, at], 1.0, 0.0)

    cos_o, sin_o = sincos_twice(oang_ref[...] * 0.5)
    orad = orad_ref[...]
    obs_x = orad * cos_o
    obs_y = orad * sin_o
    obs_z = oax_ref[...]
    mid_p = axial - 4.0
    mid_o = obs_z - 4.0
    left, right = [], []
    for mine, theirs in ((cos_p * -2.0, obs_x), (sin_p * -2.0, obs_y), (mid_p * -2.0, mid_o)):
        products(left, right, mine, theirs)
    one_p = jnp.ones((1, PTS), F32)
    one_o = jnp.ones((1, NOBS), F32)
    for piece in split3(mid_p * mid_p + 1.0):
        left.append(piece.astype(F32))
        right.append(one_o)
    for piece in split3(orad * orad + mid_o * mid_o):
        left.append(one_p)
        right.append(piece.astype(F32))
    square_ref[...] = dot_nn(jnp.concatenate(left, axis=0).T.astype(BF16), jnp.concatenate(right, axis=0).astype(BF16))
    tab_copy.wait()
    for f in range(FIELDS):
        tabt[f * NODES : (f + 1) * NODES, :] = tab[f].T

    def geometry(first, last):
        @pl.loop(first, last)
        def _(step):
            pairs_of([(step * 2 + u, g) for u in range(2) for g in range(2)])

    def pairs_of(places):
        if True:
            if True:
                for blk, g in places:
                    square = square_ref[pl.ds(pl.multiple_of(blk * 8, 8), 8), g * 128 : (g + 1) * 128]
                    inv = lax.rsqrt(square)
                    dist = square * inv
                    turns = jnp.round(dist * (0.125 / math.pi))
                    r = dist * 0.125 - turns * PI_HI - turns * PI_LO
                    c1, s1 = sincos_twice(r)
                    t = c1 + c1
                    c2 = t * c1 - 1.0
                    s2 = t * s1
                    c3 = t * c2 - c1
                    s3 = t * s2 - s1
                    c4 = t * c3 - c2
                    s4 = t * s3 - s2
                    c5 = t * c4 - c3
                    s5 = t * s4 - s3
                    t5 = c5 + c5
                    c10 = t5 * c5 - 1.0
                    s10 = t5 * s5
                    c9 = t5 * c4 - c1
                    t9 = c9 + c9
                    c19 = t9 * c10 - c1
                    s19 = t9 * s10 - s1
                    c28 = t9 * c19 - c10
                    s28 = t9 * s19 - s10
                    for n, value in enumerate(
                        (c1, s1, c2, s2, c3, s3, c4, s4, c10, s10, c19, s19, c28, s28, inv)
                    ):
                        geo[blk, g, n] = value

    geometry(0, INSIDE // 2)

    whole(req_in, 0).wait_recv()

    first = req_in[:, 0, :].T
    second = req_in[:, 1, :].T
    rid[...] = first[0:CAP]
    for n, value in enumerate((first[CAP : 2 * CAP], second[0:CAP])):
        for i, weight in enumerate(lagrange(value)):
            lag[n * 8 + i] = weight
    for i, weight in enumerate(lagrange(second[CAP : 2 * CAP])):
        lag_t[:, i, :] = weight

    elem_iota = lax.broadcasted_iota(jnp.int32, (ELEM, 128), 0).astype(F32)

    def gather(group, land, first, span):
        picks = []
        weights = []
        inner_weights = []
        for part in range(WIDE):
            c = group * WIDE + part
            picks.append(jnp.where(elem_iota == rid[pl.ds(c, 1), :], 1.0, 0.0).astype(BF16))
            weights.append([lag[n, pl.ds(c, 1), :] for n in range(16)])
            inner_weights.append(lag_t[c])
        pick = jnp.concatenate(picks, axis=1)
        weight = [jnp.concatenate([row[n] for row in weights], axis=1) for n in range(16)]
        inner_weight = jnp.concatenate(inner_weights, axis=1)
        for f in range(FIELDS):
            nodal = dot_nn(tabt[f * NODES : (f + 1) * NODES, :], pick)
            total = None
            for i in range(8):
                inner = None
                for j in range(8):
                    at = (i * 8 + j) * 8
                    term = nodal[at : at + 8, :] * weight[8 + j]
                    inner = term if inner is None else inner + term
                inner = inner * weight[i]
                total = inner if total is None else total + inner
                if i % EVERY == 0:
                    unit = f * (8 // EVERY) + i // EVERY
                    pairs_of([(INSIDE + group * (20 // EVERY) + unit // 2, unit % 2)])
            value = jnp.sum(total * inner_weight, axis=0, keepdims=True)
            for part in range(WIDE):
                land[pl.ds(f * span + (group * WIDE - first) + part, 1), :] = value[:, part * 128 : (part + 1) * 128]

    pl.loop(0, SOON // WIDE)(lambda group: gather(group, valt, 0, SOON))
    valt[FIELDS * SOON : 256, :] = jnp.zeros((256 - FIELDS * SOON, 128), F32)
    for n in range(2):
        rep_out[:, n, :] = valt[n * 128 : (n + 1) * 128, :].T
    exchange(rep_out, rep_in, 1, reply=True)
    rep_in[0] = rep_out[0]
    pl.loop(SOON // WIDE, CAP // WIDE)(lambda group: gather(group, valt_b, SOON, CAP - SOON))
    valt_b[FIELDS * (CAP - SOON) : 128, :] = jnp.zeros((128 - FIELDS * (CAP - SOON), 128), F32)
    rep_out_b[:, 0, :] = valt_b[...].T
    exchange(rep_out_b, rep_in_b, 3, reply=True)
    rep_in_b[0] = rep_out_b[0]

    def sources(landing, count):
        parts = [split2(landing[:, n, :].T) for n in range(count)]
        return jnp.concatenate(
            [
                jnp.concatenate([hi for hi, lo in parts], axis=0),
                jnp.concatenate([lo for hi, lo in parts], axis=0),
            ],
            axis=1,
        )

    def pick(table, choose, mask, span):
        found = dot_nn(table, choose)
        return [
            jnp.sum(found[f * span : (f + 1) * span, :] * mask, axis=0, keepdims=True) for f in range(FIELDS)
        ]

    def amplitudes(first, last, values):
        at_p = slice(first * BLK, last * BLK)
        density, vel_x, vel_y, vel_z, pressure = values
        cos_q, sin_q, axial_q = cos_p[:, at_p], sin_p[:, at_p], axial[:, at_p]
        normal = vel_x * cos_q + vel_y * sin_q
        scaled = panel[:, at_p] * (1.0 / math.sqrt(PTS * DEV))
        flux = density * normal * scaled
        pressure = pressure * scaled
        left, right = [], []
        products(left, right, pressure * cos_q + flux * vel_x, obs_x)
        products(left, right, pressure * sin_q + flux * vel_y, obs_y)
        products(left, right, flux * vel_z, obs_z)
        for piece in split3(-(pressure + flux * (normal + vel_z * axial_q))):
            left.append(piece.astype(F32))
            right.append(one_o)
        zero_o = jnp.zeros((1, NOBS), F32)
        other = [zero_o] * len(left)
        for piece in split3(flux):
            left.append(piece.astype(F32))
            right.append(zero_o)
            other.append(one_o)
        left = jnp.concatenate(left, axis=0).T.astype(BF16)
        right = jnp.concatenate(
            [jnp.concatenate(right, axis=0), jnp.concatenate(other, axis=0)], axis=1
        ).astype(BF16)
        for blk in range(last - first):
            mixed = dot_nn(left[blk * BLK : (blk + 1) * BLK, :], right)
            for n in range(BLK // 8):
                at = (first + blk) * (BLK // 8) + n
                for g in range(2):
                    lanes = slice(g * 128, (g + 1) * 128)
                    inv = geo[at, g, 14]
                    linear = mixed[n * 8 : n * 8 + 8, lanes]
                    amp[at, g] = (
                        mixed[n * 8 : n * 8 + 8, 256 + g * 128 : 384 + g * 128] + linear * inv
                    ) * (inv * orad[:, lanes])

    def put(k, lanes, cosine, sine):
        sums[k - 1 : k, lanes] = jnp.sum(cosine, axis=0, keepdims=True)
        sums[NFREQ + k - 1 : NFREQ + k, lanes] = jnp.sum(sine, axis=0, keepdims=True)

    def green(first, last, begin, end):
        for g in range(2):
            lanes = slice(g * 128, (g + 1) * 128)
            base = 0
            for number, (centre, reach) in enumerate(CENTRES):

                def body(step, acc, number=number, reach=reach, g=g):
                    acc = list(acc)
                    for u in range(UNROLL):
                        blk = step * UNROLL + u
                        a = amp[blk, g]
                        at = 4 if number == 0 else 6 + 2 * number
                        ac = a * geo[blk, g, at]
                        as_ = a * geo[blk, g, at + 1]
                        acc[0] = acc[0] + ac
                        acc[1] = acc[1] + as_
                        for b in range(reach):
                            yc = geo[blk, g, 2 * b]
                            ysn = geo[blk, g, 2 * b + 1]
                            acc[2 + 4 * b] = acc[2 + 4 * b] + ac * yc
                            acc[3 + 4 * b] = acc[3 + 4 * b] + as_ * ysn
                            acc[4 + 4 * b] = acc[4 + 4 * b] + as_ * yc
                            acc[5 + 4 * b] = acc[5 + 4 * b] + ac * ysn
                    return tuple(acc)

                count = 2 + 4 * reach
                if begin:
                    start = tuple(jnp.zeros((8, 128), F32) for _ in range(count))
                else:
                    start = tuple(partial[g, base + n] for n in range(count))
                acc = lax.fori_loop(first // (8 * UNROLL), last // (8 * UNROLL), body, start)
                if end:
                    put(centre, lanes, acc[0], acc[1])
                    for b in range(reach):
                        p1, p2, p3, p4 = acc[2 + 4 * b : 6 + 4 * b]
                        put(centre + b + 1, lanes, p1 - p2, p3 + p4)
                        put(centre - b - 1, lanes, p1 + p2, p3 - p4)
                else:
                    for n in range(count):
                        partial[g, base + n] = acc[n]
                base += count

    whole(rep_in, 1).wait_recv()
    table = sources(rep_in, 2)
    soon_blocks = SOON_PTS // BLK
    found = []
    for blk in range(soon_blocks):
        at = slice(blk * BLK, (blk + 1) * BLK)
        found.append(pick(table, hot_p[:, at], rankm_p[0:SOON, at], SOON))
    amplitudes(0, soon_blocks, [jnp.concatenate([row[f] for row in found], axis=1) for f in range(FIELDS)])
    green(0, SOON_PTS, True, False)
    whole(rep_in_b, 3).wait_recv()
    table_b = sources(rep_in_b, 1)
    found = []
    for blk in range(soon_blocks, PTS // BLK):
        at = slice(blk * BLK, (blk + 1) * BLK)
        found.append(
            [
                one + two
                for one, two in zip(
                    pick(table, hot_p[:, at], rankm_p[0:SOON, at], SOON),
                    pick(table_b, hot_p[:, at], rankm_p[SOON:CAP, at], CAP - SOON),
                )
            ]
        )
    amplitudes(
        soon_blocks, PTS // BLK, [jnp.concatenate([row[f] for row in found], axis=1) for f in range(FIELDS)]
    )
    green(SOON_PTS, PTS, False, True)

    slot = slot_ref[...]
    col_iota = lax.broadcasted_iota(jnp.int32, (DEV, NOBS), 0) * 2
    pieces = split3(sums[...])
    placed = []
    for parity in range(2):
        choose = jnp.where(col_iota + parity == slot, 1.0, 0.0).astype(BF16)
        placed.append(dot_nt(choose, pieces[0]) + dot_nt(choose, pieces[1]) + dot_nt(choose, pieces[2]))
    red_out[:, 0, :] = jnp.concatenate(placed, axis=1)
    exchange(red_out, red_in, 2, own=True)
    red_in[0] = red_out[me]
    cos_f, sin_f = sincos_twice(phase_ref[...] * 0.5)
    for blk in range(PTS // BLK):
        at = slice(blk * BLK, (blk + 1) * BLK)
        one = pick(table, hot[:, at], rankm[0:SOON, at], SOON)
        two = pick(table_b, hot[:, at], rankm[SOON:CAP, at], CAP - SOON)
        for f in range(FIELDS):
            surf_ref[f : f + 1, at] = one[f] + two[f]
    whole(red_in, 2).wait_recv()
    total = jnp.sum(red_in[:, 0, :], axis=0, keepdims=True)
    for parity in range(2):
        cosine = total[:, parity * 64 : parity * 64 + 32]
        sine = total[:, parity * 64 + 32 : parity * 64 + 64]
        spec_ref[0, parity : parity + 1, :] = prior_ref[0, parity : parity + 1, :] + (
            cos_f * cosine - sin_f * sine
        )
        spec_ref[1, parity : parity + 1, :] = prior_ref[1, parity : parity + 1, :] - (
            sin_f * cosine + cos_f * sine
        )
    whole(req_in, 0).wait_send()
    whole(rep_in, 1).wait_send()
    whole(rep_in_b, 3).wait_send()
    whole(red_in, 2).wait_send()


def hand_over(surface_in, spectra_in, surface_out, spectra_out, sems):
    copies = [
        pltpu.make_async_copy(surface_in, surface_out, sems.at[0]),
        pltpu.make_async_copy(spectra_in, spectra_out, sems.at[1]),
    ]
    for copy in copies:
        copy.start()
    for copy in copies:
        copy.wait()


def on_device(
    element_fields,
    ref_coords,
    local_element,
    owner,
    point_angle,
    point_axial,
    panel_weight,
    obs_radius,
    obs_angle,
    obs_axial,
    step_phase,
    observer_slot,
    prior_spectra,
):
    vmem = pl.BlockSpec(memory_space=pltpu.VMEM)
    surface, spectra = pl.pallas_call(
        kernel,
        out_shape=(pltpu.VMEM((FIELDS, PTS), F32), pltpu.VMEM((2, 2, NFREQ), F32)),
        in_specs=[pl.BlockSpec(memory_space=pltpu.HBM)] + [vmem] * 12,
        out_specs=(vmem, vmem),
        scratch_shapes=[
            pltpu.VMEM((FIELDS, ELEM, NODES), BF16),
            pltpu.VMEM((FIELDS * NODES, ELEM), BF16),
            pltpu.VMEM((2 * DEV, PTS), BF16),
            pltpu.VMEM((CAP, PTS), F32),
            pltpu.VMEM((DEV, 2, 128), F32),
            pltpu.VMEM((DEV, 2, 128), F32),
            pltpu.VMEM((CAP, 128), F32),
            pltpu.VMEM((16, CAP, 128), F32),
            pltpu.VMEM((CAP, 8, 128), F32),
            pltpu.VMEM((256, 128), F32),
            pltpu.VMEM((128, 128), F32),
            pltpu.VMEM((DEV, 2, 128), F32),
            pltpu.VMEM((DEV, 2, 128), F32),
            pltpu.VMEM((DEV, 1, 128), F32),
            pltpu.VMEM((DEV, 1, 128), F32),
            pltpu.VMEM((PTS - SOON_PTS, PTS), BF16),
            pltpu.VMEM((2 * DEV, PTS), BF16),
            pltpu.VMEM((CAP, PTS), F32),
            pltpu.VMEM((2, 66, 8, 128), F32),
            pltpu.VMEM((PTS, NOBS), F32),
            pltpu.VMEM((PTS // 8, 2, 8, 128), F32),
            pltpu.VMEM((PTS // 8, 2, 15, 8, 128), F32),
            pltpu.VMEM((2 * NFREQ, NOBS), F32),
            pltpu.VMEM((DEV, 1, 128), F32),
            pltpu.VMEM((DEV, 1, 128), F32),
            pltpu.SemaphoreType.DMA,
            pltpu.SemaphoreType.DMA((8,)),
        ],
        compiler_params=pltpu.CompilerParams(
            collective_id=0, has_side_effects=True, vmem_limit_bytes=63 * 1024 * 1024
        ),
        name="flow",
    )(
        element_fields.transpose(1, 0, 2),
        ref_coords,
        local_element.reshape(1, PTS),
        owner.reshape(1, PTS),
        point_angle.reshape(1, PTS),
        point_axial.reshape(1, PTS),
        panel_weight.reshape(1, PTS),
        obs_radius.reshape(1, NOBS),
        obs_angle.reshape(1, NOBS),
        obs_axial.reshape(1, NOBS),
        step_phase.reshape(1, NFREQ),
        observer_slot.reshape(1, NOBS),
        prior_spectra.transpose(0, 2, 1),
    )
    surface, spectra = pl.pallas_call(
        hand_over,
        out_shape=(
            jax.ShapeDtypeStruct((FIELDS, PTS), F32),
            jax.ShapeDtypeStruct((2, 2, NFREQ), F32),
        ),
        in_specs=[vmem, vmem],
        out_specs=(pl.BlockSpec(memory_space=pltpu.HBM), pl.BlockSpec(memory_space=pltpu.HBM)),
        scratch_shapes=[pltpu.SemaphoreType.DMA((2,))],
        name="hand_over",
    )(
        pltpu.with_memory_space_constraint(surface, pltpu.VMEM),
        pltpu.with_memory_space_constraint(spectra, pltpu.VMEM),
    )
    return surface, spectra.transpose(0, 2, 1)


def solution(mesh):
    return jax.shard_map(
        on_device,
        mesh=mesh,
        in_specs=(
            P(("gx", "gy"), None, None),
            P(None, ("gx", "gy")),
            P(("gx", "gy")),
            P(("gx", "gy"), None),
            P(("gx", "gy")),
            P(("gx", "gy")),
            P(("gx", "gy")),
            P(),
            P(),
            P(),
            P(),
            P(),
            P(None, None, ("gx", "gy")),
        ),
        out_specs=(P(None, ("gx", "gy")), P(None, None, ("gx", "gy"))),
        check_vma=False,
    )
```
